128 devices in a mesh: rows: 32 (over x, z, core), feat: 4 (over y).
Axes of the slice: x: 4, y: 4, z: 4, core: 2. Of those that a mesh axis runs over, the one named last changes fastest.
Arguments:
- bins: int32 [256, 49152], P('feat', 'rows'), may hold values from 0 to 255
- gradients: bfloat16 [49152], P('rows'), may hold values from -11 to 14
- hessians: bfloat16 [49152], P('rows'), may hold values from 0.099609375 to 1
- predictions: float32 [49152], P('rows'), may hold values from -6 to 6
- leaf: int32 [49152], P('rows'), may hold values from 0 to 7
- split_feature: int32 [8], replicated, may hold values from 0 to 255
- split_bin: int32 [8], replicated, may hold values from 0 to 254
- row_counts: int32 [32], P('rows'), may hold values from 96 to 1536, as said below
Outputs:
- hist: float32 [4, 64, 2, 16, 256], P('feat', 'rows')
- new_leaf: int32 [49152], P('rows')
- new_pred: float32 [49152], P('rows')
The draws below stay inside these ranges and needn't reach their ends.
Inputs may be any that keep to these rules, and one draw needn't show every extreme that they name: `row_counts`: some sweep batch has all 1536 rows live.
All inputs are finite; a program needn't handle non-finite values.
Results may differ from the reference program's by a relative error of at most 0.0003.
Values may be sent and summed in bfloat16 or wider, within the bound.
No kernel may reach another device: no remote copies, remote signals or barrier semaphores. Data moves between devices by JAX's collectives and lax.ppermute only.
A program may use at most 128 MiB of HBM per device.

```python
import math
import jax
import jax.numpy as jnp
from jax import lax

F = 256
B = 256
LEAVES = 8
ROW_CAP = 1536
ROWS = 49152
N_FEAT = 4


def draw_gradients(key, part):
    count = ROWS // ROW_CAP
    shard = (jnp.arange(ROWS) // ROW_CAP).astype(jnp.float32)
    scale = 1.0 + 2.0 * shard / max(count - 1, 1)
    base = 0.6 + jax.random.truncated_normal(key, -4.0, 4.0, (ROWS,), jnp.float32)
    return (scale * base).astype(jnp.bfloat16)


def draw_row_counts(key, part):
    count = ROWS // ROW_CAP
    first = jax.random.fold_in(key, 11)
    second = jax.random.fold_in(key, 12)
    third = jax.random.fold_in(key, 13)
    base = jax.random.randint(first, (count,), ROW_CAP // 16, ROW_CAP // 2 + 1)
    full = jax.random.randint(second, (count,), 0, 8) == 0
    picked = jax.random.randint(third, (), 0, count)
    full = full | (jnp.arange(count) == picked)
    return jnp.where(full, ROW_CAP, base).astype(jnp.int32)


def touch_ends(result, own_key, smallest, top_value):
    longest = result.shape.index(max(result.shape))
    spots = []
    for shift in (0, 1):
        where = [jax.random.randint(jax.random.fold_in(own_key, axis), (), 0, length) for axis, length in enumerate(result.shape)]
        where[longest] = (where[longest] + shift) % result.shape[longest]
        spots.append(tuple(where))
    return result.at[spots[0]].set(smallest).at[spots[1]].set(top_value)


def steps_of(rng, extent, shards, low, top_value):
    gain = 1.0
    for axis_at, blocks in shards:
        draws = jax.random.uniform(jax.random.fold_in(jax.random.fold_in(rng, 6), axis_at), (blocks,), jnp.float32, low / len(shards), top_value / len(shards))
        gain = gain * jnp.repeat(jnp.exp(draws), extent[axis_at] // blocks).reshape((-1,) + (1,) * (len(extent) - 1 - axis_at))
    return gain


def gaussian(own_key, dims, width, bound, pieces=(), held_as=jnp.bfloat16):
    factor_of = steps_of(own_key, dims, pieces, -0.22, 0.18) if pieces else 1.0
    drawn = jax.random.normal(own_key, dims, jnp.float32) * width * factor_of
    return jnp.minimum(jnp.maximum(drawn, -bound), bound).astype(held_as)


def setup_inputs(seed: int = 0) -> dict:
    key_of = jax.random.split(jax.random.key(seed), 9)
    return {
        "bins": touch_ends(jax.random.randint(key_of[0], (F, ROWS), 0, B), jax.random.fold_in(key_of[0], 1), 0, B - 1).astype(jnp.int32),
        "gradients": draw_gradients(jax.random.fold_in(key_of[8], 71), 0),
        "hessians": jnp.clip(jnp.exp(math.log(1.0) - 2.306499 * jax.random.uniform(key_of[2], (ROWS,), jnp.float32) ** steps_of(key_of[2], (ROWS,), ((0, 32),), -0.2, 0.2)), 0.099609375, 1.0).astype(jnp.bfloat16),
        "predictions": gaussian(key_of[3], (ROWS,), 1.0, 6.0, ((0, 32),), jnp.float32),
        "leaf": touch_ends(jax.random.randint(key_of[4], (ROWS,), 0, LEAVES), jax.random.fold_in(key_of[4], 1), 0, LEAVES - 1).astype(jnp.int32),
        "split_feature": touch_ends(jax.random.randint(key_of[5], (LEAVES,), 0, F), jax.random.fold_in(key_of[5], 1), 0, F - 1).astype(jnp.int32),
        "split_bin": touch_ends(jax.random.randint(key_of[6], (LEAVES,), 0, B - 1), jax.random.fold_in(key_of[6], 1), 0, (B - 1) - 1).astype(jnp.int32),
        "row_counts": draw_row_counts(jax.random.fold_in(key_of[8], 71), 0),
    }


def reference(bins, gradients, hessians, predictions, leaf, split_feature, split_bin, row_counts):
    total = bins.shape[1]
    kids = 2 * LEAVES
    position = jnp.arange(total, dtype=jnp.int32)
    batch = (position // ROW_CAP).astype(jnp.int32)
    live = (position % ROW_CAP) < row_counts[batch]
    wanted = split_feature[leaf]
    cutoff = split_bin[leaf]
    chosen = jnp.take_along_axis(bins, wanted[None, :], 0)[0]
    going = jnp.where(chosen > cutoff, 1, 0).astype(jnp.int32)
    new_leaf = (2 * leaf + going).astype(jnp.int32)
    grad_live = jnp.where(live, gradients.astype(jnp.float32), jnp.float32(0.0))
    hess_live = jnp.where(live, hessians.astype(jnp.float32), jnp.float32(0.0))
    weights = jnp.stack([grad_live, hess_live], 1)

    def one_feature(column):
        index = (new_leaf * B + column).astype(jnp.int32)
        summed = jax.ops.segment_sum(weights, index, num_segments=kids * B)
        return summed.reshape(kids, B, 2).transpose(2, 0, 1)

    hist = lax.map(one_feature, bins)
    hist = hist.reshape(N_FEAT, F // N_FEAT, 2, kids, B)
    totals = jax.ops.segment_sum(weights, new_leaf, num_segments=kids)
    value = -totals[:, 0] / (totals[:, 1] + 1.0)
    new_pred = predictions + 0.5 * value[new_leaf]
    return hist, new_leaf, new_pred
```

```python
import jax
import jax.numpy as jnp
from jax import lax
from jax.experimental import pallas as pl
from jax.experimental.pallas import tpu as pltpu
from jax.sharding import PartitionSpec as P

B = 256
LEAVES = 8
KIDS = 2 * LEAVES
LANES = 128
GROUP = 16
VMEM = pl.BlockSpec(memory_space=pltpu.VMEM)
SMALL = pltpu.CompilerParams(vmem_limit_bytes=16 << 20)
SMEM = pl.BlockSpec(memory_space=pltpu.SMEM)


def split_kernel(features, cutoffs, bins, leaf, part, packed, rows):
    width, length = bins.shape
    blocks = length // LANES
    for top in range(0, width, 8):
        for k in range(blocks):
            rows[pl.ds(top * blocks + k, 8, stride=blocks), :] = bins[top : top + 8, k * LANES : (k + 1) * LANES]
    first = lax.axis_index("feat") * width
    leaves = leaf[...]
    code = jnp.zeros((blocks, LANES), jnp.int32)
    for slot in range(LEAVES):
        local = features[slot] - first
        here = ((local >= 0) & (local < width)).astype(jnp.int32)
        chosen = rows[pl.ds(jnp.clip(local, 0, width - 1) * blocks, blocks), :]
        child = (2 * slot + (chosen > cutoffs[slot]).astype(jnp.int32)) * here
        code = jnp.where(leaves == slot, child, code)
    part[...] = code.astype(jnp.float32).astype(jnp.bfloat16)
    owners, each, _ = packed.shape
    for owner in range(owners):
        packed[owner] = rows[owner * each : (owner + 1) * each, :].astype(jnp.float32).astype(jnp.bfloat16)


def fill_kernel(count, packed, gradients, hessians, mine, one, two, three, send, new_leaf, stage):
    owners, each, _ = packed.shape
    blocks = mine.shape[0]
    code = sum(x[...].astype(jnp.float32) for x in (mine, one, two, three))
    new_leaf[...] = code.astype(jnp.int32)
    spot = lax.broadcasted_iota(jnp.int32, (blocks, LANES), 0) * LANES
    spot = spot + lax.broadcasted_iota(jnp.int32, (blocks, LANES), 1)
    live = spot < count[0]
    stage[0:blocks, :] = jnp.where(live, gradients[...].astype(jnp.float32), 0.0)
    stage[blocks : 2 * blocks, :] = jnp.where(live, hessians[...].astype(jnp.float32), 0.0)
    stage[2 * blocks : 3 * blocks, :] = code
    used = (count[0] + LANES - 1) // LANES
    rest = stage.shape[0] - 3 * blocks
    stage[3 * blocks :, :] = jnp.full((rest, LANES), used, jnp.int32).astype(jnp.float32)
    tail = stage[...].astype(jnp.bfloat16)
    for owner in range(owners):
        send[owner, 0:each, :] = packed[owner]
        send[owner, each:, :] = tail


def hist_kernel(recv, new_leaf, predictions, hist, new_pred, wide, columns, accum):
    sources, height, _ = recv.shape
    blocks = new_leaf.shape[0]
    each = recv.shape[1]
    for s in range(sources):
        wide[s * each : (s + 1) * each, :] = recv[s].astype(jnp.float32)
    place = 0
    for s in range(sources):
        for j in range(5):
            columns[j, pl.ds(place, blocks), :] = wide[s * each + j * blocks : s * each + (j + 1) * blocks, :]
        used = wide[s * each + 5 * blocks : s * each + 5 * blocks + 1, :][0, 0].astype(jnp.int32)
        place = place + used
    for j in range(5):
        columns[j, pl.ds(place, GROUP), :] = jnp.zeros((GROUP, LANES), jnp.float32)
    accum[...] = jnp.zeros(accum.shape, jnp.float32)
    slots = lax.broadcasted_iota(jnp.int32, (2 * KIDS, LANES), 0).astype(jnp.float32).astype(jnp.bfloat16)
    levels = lax.broadcasted_iota(jnp.int32, (LANES, LANES), 0).astype(jnp.float32).astype(jnp.bfloat16)
    zero = jnp.zeros((), jnp.bfloat16)
    one = jnp.ones((), jnp.bfloat16)

    def spread(row, height):
        return jnp.broadcast_to(row, (height, LANES)).astype(jnp.bfloat16)

    def step(i, carry):
        base = i * GROUP
        uppers = [[], []]
        lowers = [[], []]
        for k in range(GROUP):
            at = base + k
            grad = spread(columns[2, pl.ds(at, 1), :], 2 * KIDS)
            hess = spread(columns[3, pl.ds(at, 1), :], 2 * KIDS)
            child = columns[4, pl.ds(at, 1), :]
            for f in range(2):
                cell = columns[f, pl.ds(at, 1), :]
                high = cell >= LANES
                low = spread(jnp.where(high, cell - LANES, cell), LANES)
                slot = spread(jnp.where(high, child + KIDS, child), 2 * KIDS)
                hit = slot == slots
                uppers[f].append(jnp.concatenate([jnp.where(hit, grad, zero), jnp.where(hit, hess, zero)], 0))
                lowers[f].append(jnp.where(low == levels, one, zero))
        for f in range(2):
            upper = jnp.concatenate(uppers[f], 1)
            lower = jnp.concatenate(lowers[f], 1)
            accum[f] += lax.dot_general(upper, lower, (((1,), (1,)), ((), ())), preferred_element_type=jnp.float32)
        return carry

    lax.fori_loop(0, (place + GROUP - 1) // GROUP, step, 0)
    for f in range(2):
        for kind in range(2):
            for high in range(2):
                top = (kind * 2 + high) * KIDS
                hist[f, kind, :, high * LANES : (high + 1) * LANES] = accum[f, top : top + KIDS, :]
    sums = [jnp.sum(accum[0, top : top + KIDS, :] + accum[0, top + KIDS : top + 2 * KIDS, :], 1, keepdims=True) for top in (0, 2 * KIDS)]
    value = -sums[0] / (sums[1] + 1.0)
    kids = new_leaf[...]
    gained = jnp.zeros(kids.shape, jnp.float32)
    for c in range(KIDS):
        gained = jnp.where(kids == c, jnp.broadcast_to(value[c : c + 1, :], kids.shape), gained)
    new_pred[...] = predictions[...] + 0.5 * gained


def body(bins, gradients, hessians, predictions, leaf, split_feature, split_bin, row_counts):
    width, length = bins.shape
    blocks = length // LANES
    owners = lax.axis_size("rows")
    feats = lax.axis_size("feat")
    each = width // owners * blocks
    shape = jax.ShapeDtypeStruct
    tall = lambda x: x.reshape(blocks, LANES)
    part, packed = pl.pallas_call(
        split_kernel,
        out_shape=(shape((blocks, LANES), jnp.bfloat16), shape((owners, each, LANES), jnp.bfloat16)),
        in_specs=[SMEM, SMEM, VMEM, VMEM],
        out_specs=(VMEM, VMEM),
        scratch_shapes=[pltpu.VMEM((width * blocks, LANES), jnp.int32)],
        name="split_rows",
        compiler_params=SMALL,
    )(split_feature, split_bin, bins, tall(leaf))
    others = [lax.ppermute(part, "feat", [(i, (i + s) % feats) for i in range(feats)]) for s in range(1, feats)]
    height = each + 3 * blocks + 4
    send, new_leaf = pl.pallas_call(
        fill_kernel,
        out_shape=(shape((owners, height, LANES), jnp.bfloat16), shape((blocks, LANES), jnp.int32)),
        in_specs=[SMEM] + [VMEM] * 7,
        out_specs=(VMEM, VMEM),
        scratch_shapes=[pltpu.VMEM((height - each, LANES), jnp.float32)],
        name="fill_messages",
        compiler_params=SMALL,
    )(row_counts, packed, tall(gradients), tall(hessians), part, *others)
    recv = lax.all_to_all(send, "rows", 0, 0, tiled=True)
    hist, new_pred = pl.pallas_call(
        hist_kernel,
        out_shape=(shape((2, 2, KIDS, B), jnp.float32), shape((blocks, LANES), jnp.float32)),
        in_specs=[VMEM] * 3,
        out_specs=(VMEM, VMEM),
        scratch_shapes=[
            pltpu.VMEM((owners * height, LANES), jnp.float32),
            pltpu.VMEM((5, owners * blocks + GROUP, LANES), jnp.float32),
            pltpu.VMEM((2, 4 * KIDS, LANES), jnp.float32),
        ],
        name="histograms",
        compiler_params=SMALL,
    )(recv, new_leaf, tall(predictions))
    return (hist[None], new_leaf.reshape(-1), new_pred.reshape(-1))


def solution(mesh):
    in_specs = (P("feat", "rows"), P("rows"), P("rows"), P("rows"), P("rows"), P(), P(), P("rows"))
    out_specs = (P("feat", "rows", None, None, None), P("rows"), P("rows"))
    return jax.shard_map(body, mesh=mesh, in_specs=in_specs, out_specs=out_specs, check_vma=False)
```

```python
import jax
import jax.numpy as jnp
from jax import lax
from jax.experimental import pallas as pl
from jax.experimental.pallas import tpu as pltpu
from jax.sharding import PartitionSpec as P

B = 256
LEAVES = 8
KIDS = 2 * LEAVES
LANES = 128
GROUP = 32
LOW = jnp.float8_e4m3fn
VMEM = pl.BlockSpec(memory_space=pltpu.VMEM)
SMALL = pltpu.CompilerParams(vmem_limit_bytes=16 << 20)
SMEM = pl.BlockSpec(memory_space=pltpu.SMEM)


def split_kernel(bins, leaf, features, cutoffs, part, packed, cells, rows, leaves, wanted, limits, sems):
    width, length = bins.shape
    blocks = length // LANES
    copies = [(features, wanted), (cutoffs, limits), (leaf, leaves)]
    copies += [(bins.at[pl.ds(top, 8), :], cells.at[pl.ds(top, 8), :]) for top in range(0, width, 8)]
    copies = [pltpu.make_async_copy(source, target, sems.at[i]) for i, (source, target) in enumerate(copies)]
    for copy in copies:
        copy.start()
    for copy in copies:
        copy.wait()
    for top in range(0, width, 8):
        for k in range(blocks):
            rows[pl.ds(top * blocks + k, 8, stride=blocks), :] = cells[top : top + 8, k * LANES : (k + 1) * LANES]
    first = lax.axis_index("feat") * width
    code = jnp.zeros((blocks, LANES), jnp.int32)
    for slot in range(LEAVES):
        local = wanted[slot] - first
        here = ((local >= 0) & (local < width)).astype(jnp.int32)
        chosen = rows[pl.ds(jnp.clip(local, 0, width - 1) * blocks, blocks), :]
        child = (2 * slot + (chosen > limits[slot]).astype(jnp.int32)) * here
        code = jnp.where(leaves[...] == slot, child, code)
    part[...] = code.astype(jnp.float32).astype(jnp.bfloat16)
    owners, each, _ = packed.shape
    for owner in range(owners):
        packed[owner] = rows[owner * each : (owner + 1) * each, :].astype(jnp.float32).astype(jnp.bfloat16)


def fill_kernel(count, packed, gradients, hessians, mine, one, two, three, send, code, stage):
    owners, each, _ = packed.shape
    blocks = mine.shape[0]
    total = sum(x[...].astype(jnp.float32) for x in (mine, one, two, three))
    code[...] = total.astype(jnp.int32)
    spot = lax.broadcasted_iota(jnp.int32, (blocks, LANES), 0) * LANES
    spot = spot + lax.broadcasted_iota(jnp.int32, (blocks, LANES), 1)
    live = spot < count[0]
    stage[0:blocks, :] = jnp.where(live, gradients[...].astype(jnp.float32), 0.0)
    stage[blocks : 2 * blocks, :] = jnp.where(live, hessians[...].astype(jnp.float32), 0.0)
    stage[2 * blocks : 3 * blocks, :] = total
    used = (count[0] + LANES - 1) // LANES
    rest = stage.shape[0] - 3 * blocks
    stage[3 * blocks :, :] = jnp.full((rest, LANES), used, jnp.int32).astype(jnp.float32)
    tail = stage[...].astype(jnp.bfloat16)
    for owner in range(owners):
        send[owner, 0:each, :] = packed[owner]
        send[owner, each:, :] = tail


def hist_kernel(recv, code, predictions, hist, new_leaf, new_pred, wide, columns):
    pl.run_scoped(
        lambda *accs: hist_steps(recv, code, predictions, hist, new_leaf, new_pred, wide, columns, accs),
        pltpu.ACC(0)((8 * KIDS, B), jnp.float32),
        pltpu.ACC(1)((8 * KIDS, B), jnp.float32),
    )


def hist_steps(recv, code, predictions, hist, new_leaf, new_pred, wide, columns, accs):
    sources, height, _ = recv.shape
    blocks = code.shape[0]
    each = recv.shape[1]
    for acc in accs:
        pltpu.matmul_pop(acc)
    for s in range(sources):
        wide[s * each : (s + 1) * each, :] = recv[s].astype(jnp.float32)
    place = 0
    for s in range(sources):
        for j in range(5):
            columns[j, pl.ds(place, blocks), :] = wide[s * each + j * blocks : s * each + (j + 1) * blocks, :]
        used = wide[s * each + 5 * blocks : s * each + 5 * blocks + 1, :][0, 0].astype(jnp.int32)
        place = place + used
    for j in range(5):
        columns[j, pl.ds(place, GROUP), :] = jnp.zeros((GROUP, LANES), jnp.float32)
    slots = lax.broadcasted_iota(jnp.int32, (2 * KIDS, LANES), 0).astype(jnp.float32).astype(jnp.bfloat16)
    levels = lax.broadcasted_iota(jnp.int32, (LANES, LANES), 0).astype(jnp.float32).astype(jnp.bfloat16)
    zero = jnp.zeros((), jnp.bfloat16)
    one = jnp.ones((), jnp.bfloat16)

    def spread(row, height):
        return jnp.broadcast_to(row, (height, LANES)).astype(jnp.bfloat16)

    def block(at):
        grad = spread(columns[2, pl.ds(at, 1), :], 2 * KIDS)
        hess = spread(columns[3, pl.ds(at, 1), :], 2 * KIDS)
        child = columns[4, pl.ds(at, 1), :]
        upper = []
        lower = []
        for f in range(2):
            cell = columns[f, pl.ds(at, 1), :]
            high = cell >= LANES
            low = spread(jnp.where(high, cell - LANES, cell), LANES)
            slot = spread(jnp.where(high, child + KIDS, child), 2 * KIDS)
            hit = slot == slots
            upper += [jnp.where(hit, grad, zero), jnp.where(hit, hess, zero)]
            lower.append(jnp.where(low == levels, one, zero))
        return jnp.concatenate(upper, 0), jnp.concatenate(lower, 0)

    def step(i, carry):
        base = i * GROUP
        for k in range(0, GROUP, 2):
            first, second = block(base + k), block(base + k + 1)
            upper = jnp.concatenate([first[0], second[0]], 1)
            lower = jnp.concatenate([first[1], second[1]], 1).astype(LOW)
            unit, slot = (k // 2) % 2, (k // 4) % 2
            pltpu.matmul_push_rhs(lower, staging_register=slot, mxu_index=unit, transpose=True)
            pltpu.matmul_acc_lhs(accs[unit], upper, load_staged_rhs=slot)
        return carry

    lax.fori_loop(0, (place + GROUP - 1) // GROUP, step, 0)
    total = pltpu.matmul_pop(accs[0]) + pltpu.matmul_pop(accs[1])
    for f in range(2):
        mine = total[f * 4 * KIDS : (f + 1) * 4 * KIDS, f * LANES : (f + 1) * LANES]
        for kind in range(2):
            for high in range(2):
                top = (kind * 2 + high) * KIDS
                hist[f, kind, :, high * LANES : (high + 1) * LANES] = mine[top : top + KIDS, :]
        if f == 0:
            sums = [jnp.sum(mine[top : top + KIDS, :] + mine[top + KIDS : top + 2 * KIDS, :], 1, keepdims=True) for top in (0, 2 * KIDS)]
    value = -sums[0] / (sums[1] + 1.0)
    kids = code[...]
    new_leaf[...] = kids
    gained = jnp.zeros(kids.shape, jnp.float32)
    for c in range(KIDS):
        gained = jnp.where(kids == c, jnp.broadcast_to(value[c : c + 1, :], kids.shape), gained)
    new_pred[...] = predictions[...] + 0.5 * gained


def body(bins, gradients, hessians, predictions, leaf, split_feature, split_bin, row_counts):
    width, length = bins.shape
    blocks = length // LANES
    owners = lax.axis_size("rows")
    feats = lax.axis_size("feat")
    each = width // owners * blocks
    shape = jax.ShapeDtypeStruct
    tall = lambda x: x.reshape(blocks, LANES)
    here = pl.BlockSpec(memory_space=pltpu.HBM)
    height = each + 3 * blocks + 4
    part, packed = pl.pallas_call(
        split_kernel,
        out_shape=(shape((blocks, LANES), jnp.bfloat16), shape((owners, each, LANES), jnp.bfloat16)),
        in_specs=[here] * 4,
        out_specs=(VMEM, VMEM),
        scratch_shapes=[
            pltpu.VMEM((width, length), jnp.int32),
            pltpu.VMEM((width * blocks, LANES), jnp.int32),
            pltpu.VMEM((blocks, LANES), jnp.int32),
            pltpu.SMEM((LEAVES,), jnp.int32),
            pltpu.SMEM((LEAVES,), jnp.int32),
            pltpu.SemaphoreType.DMA((3 + width // 8,)),
        ],
        name="split_rows",
        compiler_params=SMALL,
    )(*(pltpu.with_memory_space_constraint(x, pltpu.HBM) for x in (bins, tall(leaf), split_feature, split_bin)))
    others = [lax.ppermute(part, "feat", [(i, (i + s) % feats) for i in range(feats)]) for s in range(1, feats)]
    send, code = pl.pallas_call(
        fill_kernel,
        out_shape=(shape((owners, height, LANES), jnp.bfloat16), shape((blocks, LANES), jnp.int32)),
        in_specs=[SMEM] + [VMEM] * 7,
        out_specs=(VMEM, VMEM),
        scratch_shapes=[pltpu.VMEM((height - each, LANES), jnp.float32)],
        name="fill_messages",
        compiler_params=SMALL,
    )(row_counts, packed, tall(gradients), tall(hessians), part, *others)
    recv = lax.all_to_all(send, "rows", 0, 0, tiled=True)
    hist, new_leaf, new_pred = pl.pallas_call(
        hist_kernel,
        out_shape=(shape((2, 2, KIDS, B), jnp.float32), shape((blocks, LANES), jnp.int32), shape((blocks, LANES), jnp.float32)),
        in_specs=[VMEM] * 3,
        out_specs=(VMEM, VMEM, VMEM),
        scratch_shapes=[
            pltpu.VMEM((owners * height, LANES), jnp.float32),
            pltpu.VMEM((5, owners * blocks + GROUP, LANES), jnp.float32),
        ],
        name="histograms",
        compiler_params=SMALL,
    )(recv, code, tall(predictions))
    return (hist[None], new_leaf.reshape(-1), new_pred.reshape(-1))


def solution(mesh):
    in_specs = (P("feat", "rows"), P("rows"), P("rows"), P("rows"), P("rows"), P(), P(), P("rows"))
    out_specs = (P("feat", "rows", None, None, None), P("rows"), P("rows"))
    return jax.shard_map(body, mesh=mesh, in_specs=in_specs, out_specs=out_specs, check_vma=False)
```

```python
import jax
import jax.numpy as jnp
from jax import lax
from jax.experimental import pallas as pl
from jax.experimental.pallas import tpu as pltpu
from jax.sharding import PartitionSpec as P

B = 256
LEAVES = 8
KIDS = 2 * LEAVES
LANES = 128
GROUP = 32
LOW = jnp.float8_e4m3fn
VMEM = pl.BlockSpec(memory_space=pltpu.VMEM)
SMALL = pltpu.CompilerParams(vmem_limit_bytes=16 << 20)
SMEM = pl.BlockSpec(memory_space=pltpu.SMEM)


def split_kernel(bins, leaf, features, cutoffs, part, packed, cells, rows, leaves, wanted, limits, sems):
    width, length = bins.shape
    blocks = length // LANES
    copies = [(features, wanted), (cutoffs, limits), (leaf, leaves)]
    copies += [(bins.at[pl.ds(top, 8), :], cells.at[pl.ds(top, 8), :]) for top in range(0, width, 8)]
    copies = [pltpu.make_async_copy(source, target, sems.at[i]) for i, (source, target) in enumerate(copies)]
    for copy in copies:
        copy.start()
    for copy in copies:
        copy.wait()
    for top in range(0, width, 8):
        for k in range(blocks):
            rows[pl.ds(top * blocks + k, 8, stride=blocks), :] = cells[top : top + 8, k * LANES : (k + 1) * LANES]
    first = lax.axis_index("feat") * width
    code = jnp.zeros((blocks, LANES), jnp.int32)
    for slot in range(LEAVES):
        local = wanted[slot] - first
        here = ((local >= 0) & (local < width)).astype(jnp.int32)
        chosen = rows[pl.ds(jnp.clip(local, 0, width - 1) * blocks, blocks), :]
        child = (2 * slot + (chosen > limits[slot]).astype(jnp.int32)) * here
        code = jnp.where(leaves[...] == slot, child, code)
    part[...] = code.astype(jnp.float32).astype(jnp.bfloat16)
    owners, each, _ = packed.shape
    for owner in range(owners):
        packed[owner] = rows[owner * each : (owner + 1) * each, :].astype(jnp.float32).astype(jnp.bfloat16)


def fill_kernel(count, packed, gradients, hessians, mine, one, two, three, send, code, stage):
    owners, each, _ = packed.shape
    blocks = mine.shape[0]
    total = sum(x[...].astype(jnp.float32) for x in (mine, one, two, three))
    code[...] = total.astype(jnp.int32)
    spot = lax.broadcasted_iota(jnp.int32, (blocks, LANES), 0) * LANES
    spot = spot + lax.broadcasted_iota(jnp.int32, (blocks, LANES), 1)
    live = spot < count[0]
    stage[0:blocks, :] = jnp.where(live, gradients[...].astype(jnp.float32), 0.0)
    stage[blocks : 2 * blocks, :] = jnp.where(live, hessians[...].astype(jnp.float32), 0.0)
    stage[2 * blocks : 3 * blocks, :] = total
    used = (count[0] + LANES - 1) // LANES
    rest = stage.shape[0] - 3 * blocks
    stage[3 * blocks :, :] = jnp.full((rest, LANES), used, jnp.int32).astype(jnp.float32)
    tail = stage[...].astype(jnp.bfloat16)
    for owner in range(owners):
        send[owner, 0:each, :] = packed[owner]
        send[owner, each:, :] = tail


def hist_kernel(recv, code, predictions, hist, new_leaf, new_pred, wide, columns):
    pl.run_scoped(
        lambda *accs: hist_steps(recv, code, predictions, hist, new_leaf, new_pred, wide, columns, accs),
        pltpu.ACC(0)((8 * KIDS, B), jnp.float32),
        pltpu.ACC(1)((8 * KIDS, B), jnp.float32),
    )


def hist_steps(recv, code, predictions, hist, new_leaf, new_pred, wide, columns, accs):
    sources, height, _ = recv.shape
    blocks = code.shape[0]
    each = recv.shape[1]
    for acc in accs:
        pltpu.matmul_pop(acc)
    for s in range(sources):
        wide[s * each : (s + 1) * each, :] = recv[s].astype(jnp.float32)
    place = 0
    for s in range(sources):
        for j in range(5):
            columns[j, pl.ds(place, blocks), :] = wide[s * each + j * blocks : s * each + (j + 1) * blocks, :]
        used = wide[s * each + 5 * blocks : s * each + 5 * blocks + 1, :][0, 0].astype(jnp.int32)
        place = place + used
    for j in range(5):
        columns[j, pl.ds(place, GROUP), :] = jnp.zeros((GROUP, LANES), jnp.float32)
    slots = lax.broadcasted_iota(jnp.int32, (2 * KIDS, LANES), 0).astype(jnp.float32).astype(jnp.bfloat16)
    levels = lax.broadcasted_iota(jnp.int32, (LANES, LANES), 0).astype(jnp.float32).astype(jnp.bfloat16)
    zero = jnp.zeros((), jnp.bfloat16)
    one = jnp.ones((), jnp.bfloat16)

    def spread(row, height):
        return jnp.broadcast_to(row, (height, LANES)).astype(jnp.bfloat16)

    def block(at):
        grad = spread(columns[2, pl.ds(at, 1), :], 2 * KIDS)
        hess = spread(columns[3, pl.ds(at, 1), :], 2 * KIDS)
        child = columns[4, pl.ds(at, 1), :]
        upper = []
        lower = []
        for f in range(2):
            cell = columns[f, pl.ds(at, 1), :]
            high = cell >= LANES
            low = spread(jnp.where(high, cell - LANES, cell), LANES)
            slot = spread(jnp.where(high, child + KIDS, child), 2 * KIDS)
            hit = slot == slots
            upper += [jnp.where(hit, grad, zero), jnp.where(hit, hess, zero)]
            lower.append(jnp.where(low == levels, one, zero))
        return jnp.concatenate(upper, 0), jnp.concatenate(lower, 0)

    def step(i, carry):
        base = i * GROUP
        for k in range(0, GROUP, 2):
            first, second = block(base + k), block(base + k + 1)
            upper = jnp.concatenate([first[0], second[0]], 1)
            lower = jnp.concatenate([first[1], second[1]], 1).astype(LOW)
            unit, slot = (k // 2) % 2, (k // 4) % 2
            pltpu.matmul_push_rhs(lower, staging_register=slot, mxu_index=unit, transpose=True)
            pltpu.matmul_acc_lhs(accs[unit], upper, load_staged_rhs=slot)
        return carry

    lax.fori_loop(0, (place + GROUP - 1) // GROUP, step, 0)
    total = pltpu.matmul_pop(accs[0]) + pltpu.matmul_pop(accs[1])
    for f in range(2):
        mine = total[f * 4 * KIDS : (f + 1) * 4 * KIDS, f * LANES : (f + 1) * LANES]
        for kind in range(2):
            for high in range(2):
                top = (kind * 2 + high) * KIDS
                hist[f, kind, :, high * LANES : (high + 1) * LANES] = mine[top : top + KIDS, :]
        if f == 0:
            sums = [jnp.sum(mine[top : top + KIDS, :] + mine[top + KIDS : top + 2 * KIDS, :], 1, keepdims=True) for top in (0, 2 * KIDS)]
    value = -sums[0] / (sums[1] + 1.0)
    kids = code[...]
    new_leaf[...] = kids
    gained = jnp.zeros(kids.shape, jnp.float32)
    for c in range(KIDS):
        gained = jnp.where(kids == c, jnp.broadcast_to(value[c : c + 1, :], kids.shape), gained)
    new_pred[...] = predictions[...] + 0.5 * gained


def body(bins, gradients, hessians, predictions, leaf, split_feature, split_bin, row_counts):
    width, length = bins.shape
    blocks = length // LANES
    owners = lax.axis_size("rows")
    feats = lax.axis_size("feat")
    each = width // owners * blocks
    shape = jax.ShapeDtypeStruct
    tall = lambda x: x.reshape(blocks, LANES)
    here = pl.BlockSpec(memory_space=pltpu.HBM)
    height = each + 3 * blocks + 4
    part, packed = pl.pallas_call(
        split_kernel,
        out_shape=(shape((blocks, LANES), jnp.bfloat16), shape((owners, each, LANES), jnp.bfloat16)),
        in_specs=[here] * 4,
        out_specs=(VMEM, VMEM),
        scratch_shapes=[
            pltpu.VMEM((width, length), jnp.int32),
            pltpu.VMEM((width * blocks, LANES), jnp.int32),
            pltpu.VMEM((blocks, LANES), jnp.int32),
            pltpu.SMEM((LEAVES,), jnp.int32),
            pltpu.SMEM((LEAVES,), jnp.int32),
            pltpu.SemaphoreType.DMA((3 + width // 8,)),
        ],
        name="split_rows",
        compiler_params=SMALL,
    )(*(pltpu.with_memory_space_constraint(x, pltpu.HBM) for x in (bins, tall(leaf), split_feature, split_bin)))
    others = [lax.ppermute(part, "feat", [(i, (i + s) % feats) for i in range(feats)]) for s in (3, 1, 2)]
    send, code = pl.pallas_call(
        fill_kernel,
        out_shape=(shape((owners, height, LANES), jnp.bfloat16), shape((blocks, LANES), jnp.int32)),
        in_specs=[SMEM] + [VMEM] * 7,
        out_specs=(VMEM, VMEM),
        scratch_shapes=[pltpu.VMEM((height - each, LANES), jnp.float32)],
        name="fill_messages",
        compiler_params=SMALL,
    )(row_counts, packed, tall(gradients), tall(hessians), part, *others)
    recv = lax.all_to_all(send, "rows", 0, 0, tiled=True)
    hist, new_leaf, new_pred = pl.pallas_call(
        hist_kernel,
        out_shape=(shape((2, 2, KIDS, B), jnp.float32), shape((blocks, LANES), jnp.int32), shape((blocks, LANES), jnp.float32)),
        in_specs=[VMEM] * 3,
        out_specs=(VMEM, VMEM, VMEM),
        scratch_shapes=[
            pltpu.VMEM((owners * height, LANES), jnp.float32),
            pltpu.VMEM((5, owners * blocks + GROUP, LANES), jnp.float32),
        ],
        name="histograms",
        compiler_params=SMALL,
    )(recv, code, tall(predictions))
    return (hist[None], new_leaf.reshape(-1), new_pred.reshape(-1))


def solution(mesh):
    in_specs = (P("feat", "rows"), P("rows"), P("rows"), P("rows"), P("rows"), P(), P(), P("rows"))
    out_specs = (P("feat", "rows", None, None, None), P("rows"), P("rows"))
    return jax.shard_map(body, mesh=mesh, in_specs=in_specs, out_specs=out_specs, check_vma=False)
```

```python
import jax
import jax.numpy as jnp
from jax import lax
from jax.experimental import pallas as pl
from jax.experimental.pallas import tpu as pltpu
from jax.sharding import PartitionSpec as P

B = 256
LEAVES = 8
KIDS = 2 * LEAVES
LANES = 128
GROUP = 16
LOW = jnp.float8_e4m3fn
VMEM = pl.BlockSpec(memory_space=pltpu.VMEM)
SMALL = pltpu.CompilerParams(vmem_limit_bytes=16 << 20)
SMEM = pl.BlockSpec(memory_space=pltpu.SMEM)


def split_kernel(bins, leaf, features, cutoffs, part, packed, cells, rows, leaves, wanted, limits, sems):
    width, length = bins.shape
    blocks = length // LANES
    copies = [(features, wanted), (cutoffs, limits), (leaf, leaves)]
    copies += [(bins.at[pl.ds(top, 8), :], cells.at[pl.ds(top, 8), :]) for top in range(0, width, 8)]
    copies = [pltpu.make_async_copy(source, target, sems.at[i]) for i, (source, target) in enumerate(copies)]
    for copy in copies:
        copy.start()
    for copy in copies:
        copy.wait()
    for top in range(0, width, 8):
        for k in range(blocks):
            rows[pl.ds(top * blocks + k, 8, stride=blocks), :] = cells[top : top + 8, k * LANES : (k + 1) * LANES]
    first = lax.axis_index("feat") * width
    code = jnp.zeros((blocks, LANES), jnp.int32)
    for slot in range(LEAVES):
        local = wanted[slot] - first
        here = ((local >= 0) & (local < width)).astype(jnp.int32)
        chosen = rows[pl.ds(jnp.clip(local, 0, width - 1) * blocks, blocks), :]
        child = (2 * slot + (chosen > limits[slot]).astype(jnp.int32)) * here
        code = jnp.where(leaves[...] == slot, child, code)
    part[...] = code.astype(jnp.float32).astype(jnp.bfloat16)
    owners, each, _ = packed.shape
    half = blocks // 2
    for owner in range(owners):
        order = [(parity, top) for parity in (owner % 2, 1 - owner % 2) for top in range(owner * each, (owner + 1) * each, blocks)]
        picked = [rows[pl.ds(top + parity, half, stride=2), :].astype(jnp.float32) for parity, top in order]
        packed[owner] = jnp.concatenate(picked, 0).astype(jnp.bfloat16)


def fill_kernel(count, packed, gradients, hessians, mine, one, two, three, send, code, stage):
    owners, each, _ = packed.shape
    blocks = mine.shape[0]
    half = blocks // 2
    total = sum(x[...].astype(jnp.float32) for x in (mine, one, two, three))
    code[...] = total.astype(jnp.int32)
    spot = lax.broadcasted_iota(jnp.int32, (blocks, LANES), 0) * LANES
    spot = spot + lax.broadcasted_iota(jnp.int32, (blocks, LANES), 1)
    live = spot < count[0]
    used = (count[0] + LANES - 1) // LANES
    stage[0:blocks, :] = jnp.where(live, gradients[...].astype(jnp.float32), 0.0)
    stage[blocks : 2 * blocks, :] = jnp.where(live, hessians[...].astype(jnp.float32), 0.0)
    stage[2 * blocks : 3 * blocks, :] = total
    stage[3 * blocks :, :] = jnp.full((blocks, LANES), used, jnp.int32).astype(jnp.float32)
    tails = []
    for core in range(2):
        rows = [stage[pl.ds(j * blocks + core, half, stride=2), :] for j in range(4)]
        tails.append(jnp.concatenate(rows, 0).astype(jnp.bfloat16))
    for owner in range(owners):
        send[owner, 0:each, :] = packed[owner]
        send[owner, each:, :] = tails[owner % 2]


def accumulate(cells, first, weights, counts, wide, columns, accs):
    sources, each, _ = cells.shape
    half = each // 8
    for acc in accs:
        pltpu.matmul_pop(acc)
    place = 0
    for s in range(sources):
        wide[s * each : s * each + each // 2, :] = cells[s, : each // 2, :].astype(jnp.float32)
        wide[s * each + each // 2 : (s + 1) * each, :] = weights[s, each // 2 :, :].astype(jnp.float32)
    for s in range(sources):
        for j, top in enumerate((first, first + half, 4 * half, 5 * half, 6 * half)):
            columns[j, pl.ds(place, half), :] = wide[s * each + top : s * each + top + half, :]
        used = wide[s * each + 7 * half : s * each + 7 * half + 1, :][0, 0].astype(jnp.int32)
        place = place + counts(used)
    for j in range(5):
        columns[j, pl.ds(place, GROUP), :] = jnp.zeros((GROUP, LANES), jnp.float32)
    slots = lax.broadcasted_iota(jnp.int32, (2 * KIDS, LANES), 0).astype(jnp.float32).astype(jnp.bfloat16)
    levels = lax.broadcasted_iota(jnp.int32, (LANES, LANES), 0).astype(jnp.float32).astype(jnp.bfloat16)
    zero = jnp.zeros((), jnp.bfloat16)
    one = jnp.ones((), jnp.bfloat16)

    def spread(row, height):
        return jnp.broadcast_to(row, (height, LANES)).astype(jnp.bfloat16)

    def block(at):
        grad = spread(columns[2, pl.ds(at, 1), :], 2 * KIDS)
        hess = spread(columns[3, pl.ds(at, 1), :], 2 * KIDS)
        child = columns[4, pl.ds(at, 1), :]
        upper = []
        lower = []
        for f in range(2):
            cell = columns[f, pl.ds(at, 1), :]
            high = cell >= LANES
            low = spread(jnp.where(high, cell - LANES, cell), LANES)
            slot = spread(jnp.where(high, child + KIDS, child), 2 * KIDS)
            hit = slot == slots
            upper += [jnp.where(hit, grad, zero), jnp.where(hit, hess, zero)]
            lower.append(jnp.where(low == levels, one, zero))
        return jnp.concatenate(upper, 0), jnp.concatenate(lower, 0)

    def step(i, carry):
        base = i * GROUP
        for k in range(0, GROUP, 2):
            first, second = block(base + k), block(base + k + 1)
            upper = jnp.concatenate([first[0], second[0]], 1)
            lower = jnp.concatenate([first[1], second[1]], 1).astype(LOW)
            unit, slot = (k // 2) % 2, (k // 4) % 2
            pltpu.matmul_push_rhs(lower, staging_register=slot, mxu_index=unit, transpose=True)
            pltpu.matmul_acc_lhs(accs[unit], upper, load_staged_rhs=slot)
        return carry

    lax.fori_loop(0, (place + GROUP - 1) // GROUP, step, 0)
    return pltpu.matmul_pop(accs[0]) + pltpu.matmul_pop(accs[1])


def scoped(steps):
    pl.run_scoped(
        lambda *accs: steps(accs),
        pltpu.ACC(0)((8 * KIDS, B), jnp.float32),
        pltpu.ACC(1)((8 * KIDS, B), jnp.float32),
    )


def first_kernel(recv, partial, wide, columns):
    core = lax.rem(lax.axis_index("rows"), 2)

    def steps(accs):
        total = accumulate(recv, 0, recv, lambda used: (used + 1 - core) >> 1, wide, columns, accs)
        for f in range(2):
            partial[f] = total[f * 4 * KIDS : (f + 1) * 4 * KIDS, f * LANES : (f + 1) * LANES]

    scoped(steps)


def last_kernel(recv, other, partial, code, predictions, hist, new_leaf, new_pred, wide, columns):
    core = lax.rem(lax.axis_index("rows"), 2)

    def steps(accs):
        total = accumulate(recv, recv.shape[1] // 4, other, lambda used: (used + core) >> 1, wide, columns, accs)
        for f in range(2):
            mine = partial[f] + total[f * 4 * KIDS : (f + 1) * 4 * KIDS, f * LANES : (f + 1) * LANES]
            for kind in range(2):
                for high in range(2):
                    top = (kind * 2 + high) * KIDS
                    hist[f, kind, :, high * LANES : (high + 1) * LANES] = mine[top : top + KIDS, :]
            if f == 0:
                sums = [jnp.sum(mine[top : top + KIDS, :] + mine[top + KIDS : top + 2 * KIDS, :], 1, keepdims=True) for top in (0, 2 * KIDS)]
        value = -sums[0] / (sums[1] + 1.0)
        leaves = code[...]
        new_leaf[...] = leaves
        gained = jnp.zeros(leaves.shape, jnp.float32)
        for c in range(KIDS):
            gained = jnp.where(leaves == c, jnp.broadcast_to(value[c : c + 1, :], leaves.shape), gained)
        new_pred[...] = predictions[...] + 0.5 * gained

    scoped(steps)


def body(bins, gradients, hessians, predictions, leaf, split_feature, split_bin, row_counts):
    width, length = bins.shape
    blocks = length // LANES
    owners = lax.axis_size("rows")
    feats = lax.axis_size("feat")
    each = width // owners * blocks
    shape = jax.ShapeDtypeStruct
    tall = lambda x: x.reshape(blocks, LANES)
    here = pl.BlockSpec(memory_space=pltpu.HBM)
    height = 2 * each
    wide = pltpu.VMEM((owners * height, LANES), jnp.float32)
    columns = pltpu.VMEM((5, owners * blocks // 2 + GROUP, LANES), jnp.float32)
    part, packed = pl.pallas_call(
        split_kernel,
        out_shape=(shape((blocks, LANES), jnp.bfloat16), shape((owners, each, LANES), jnp.bfloat16)),
        in_specs=[here] * 4,
        out_specs=(VMEM, VMEM),
        scratch_shapes=[
            pltpu.VMEM((width, length), jnp.int32),
            pltpu.VMEM((width * blocks, LANES), jnp.int32),
            pltpu.VMEM((blocks, LANES), jnp.int32),
            pltpu.SMEM((LEAVES,), jnp.int32),
            pltpu.SMEM((LEAVES,), jnp.int32),
            pltpu.SemaphoreType.DMA((3 + width // 8,)),
        ],
        name="split_rows",
        compiler_params=SMALL,
    )(*(pltpu.with_memory_space_constraint(x, pltpu.HBM) for x in (bins, tall(leaf), split_feature, split_bin)))
    others = [lax.ppermute(part, "feat", [(i, (i + s) % feats) for i in range(feats)]) for s in (3, 1, 2)]
    send, code = pl.pallas_call(
        fill_kernel,
        out_shape=(shape((owners, height, LANES), jnp.bfloat16), shape((blocks, LANES), jnp.int32)),
        in_specs=[SMEM] + [VMEM] * 7,
        out_specs=(VMEM, VMEM),
        scratch_shapes=[pltpu.VMEM((4 * blocks, LANES), jnp.float32)],
        name="fill_messages",
        compiler_params=SMALL,
    )(row_counts, packed, tall(gradients), tall(hessians), part, *others)
    recv = lax.all_to_all(send, "rows", 0, 0, tiled=True)
    other = lax.ppermute(recv, "rows", [(i, i ^ 1) for i in range(owners)])
    partial = pl.pallas_call(
        first_kernel,
        out_shape=shape((2, 4 * KIDS, LANES), jnp.float32),
        in_specs=[VMEM],
        out_specs=VMEM,
        scratch_shapes=[wide, columns],
        name="first_half",
        cost_estimate=pl.CostEstimate(flops=1 << 30, transcendentals=0, bytes_accessed=1 << 20),
        compiler_params=SMALL,
    )(recv)
    hist, new_leaf, new_pred = pl.pallas_call(
        last_kernel,
        out_shape=(shape((2, 2, KIDS, B), jnp.float32), shape((blocks, LANES), jnp.int32), shape((blocks, LANES), jnp.float32)),
        in_specs=[VMEM] * 5,
        out_specs=(VMEM, VMEM, VMEM),
        scratch_shapes=[wide, columns],
        name="histograms",
        compiler_params=SMALL,
    )(recv, other, partial, code, tall(predictions))
    return (hist[None], new_leaf.reshape(-1), new_pred.reshape(-1))


def solution(mesh):
    in_specs = (P("feat", "rows"), P("rows"), P("rows"), P("rows"), P("rows"), P(), P(), P("rows"))
    out_specs = (P("feat", "rows", None, None, None), P("rows"), P("rows"))
    return jax.shard_map(body, mesh=mesh, in_specs=in_specs, out_specs=out_specs, check_vma=False)
```

```python
import jax
import jax.numpy as jnp
from jax import lax
from jax.experimental import pallas as pl
from jax.experimental.pallas import tpu as pltpu
from jax.sharding import PartitionSpec as P

B = 256
LEAVES = 8
KIDS = 2 * LEAVES
LANES = 128
GROUP = 16
LOW = jnp.float8_e4m3fn
VMEM = pl.BlockSpec(memory_space=pltpu.VMEM)
SMALL = pltpu.CompilerParams(vmem_limit_bytes=16 << 20)
SMEM = pl.BlockSpec(memory_space=pltpu.SMEM)


def split_kernel(bins, leaf, features, cutoffs, part, packed, cells, rows, leaves, wanted, limits, sems):
    width, length = bins.shape
    blocks = length // LANES
    copies = [(features, wanted), (cutoffs, limits), (leaf, leaves)]
    copies += [(bins.at[pl.ds(top, 8), :], cells.at[pl.ds(top, 8), :]) for top in range(0, width, 8)]
    copies = [pltpu.make_async_copy(source, target, sems.at[i]) for i, (source, target) in enumerate(copies)]
    for copy in copies:
        copy.start()
    for copy in copies:
        copy.wait()
    for top in range(0, width, 8):
        for k in range(blocks):
            rows[pl.ds(top * blocks + k, 8, stride=blocks), :] = cells[top : top + 8, k * LANES : (k + 1) * LANES]
    first = lax.axis_index("feat") * width
    code = jnp.zeros((blocks, LANES), jnp.int32)
    for slot in range(LEAVES):
        local = wanted[slot] - first
        here = ((local >= 0) & (local < width)).astype(jnp.int32)
        chosen = rows[pl.ds(jnp.clip(local, 0, width - 1) * blocks, blocks), :]
        child = (2 * slot + (chosen > limits[slot]).astype(jnp.int32)) * here
        code = jnp.where(leaves[...] == slot, child, code)
    part[...] = code.astype(jnp.float32).astype(jnp.bfloat16)
    owners, each, _ = packed.shape
    half = blocks // 2
    for owner in range(owners):
        order = [(parity, top) for parity in (owner % 2, 1 - owner % 2) for top in range(owner * each, (owner + 1) * each, blocks)]
        picked = [rows[pl.ds(top + parity, half, stride=2), :].astype(jnp.float32) for parity, top in order]
        packed[owner] = jnp.concatenate(picked, 0).astype(jnp.bfloat16)


def fill_kernel(count, packed, gradients, hessians, mine, one, two, three, send, code, stage):
    owners, each, _ = packed.shape
    blocks = mine.shape[0]
    half = blocks // 2
    total = sum(x[...].astype(jnp.float32) for x in (mine, one, two, three))
    code[...] = total.astype(jnp.int32)
    spot = lax.broadcasted_iota(jnp.int32, (blocks, LANES), 0) * LANES
    spot = spot + lax.broadcasted_iota(jnp.int32, (blocks, LANES), 1)
    live = spot < count[0]
    used = (count[0] + LANES - 1) // LANES
    stage[0:blocks, :] = jnp.where(live, gradients[...].astype(jnp.float32), 0.0)
    stage[blocks : 2 * blocks, :] = jnp.where(live, hessians[...].astype(jnp.float32), 0.0)
    stage[2 * blocks : 3 * blocks, :] = total
    stage[3 * blocks :, :] = jnp.full((blocks, LANES), used, jnp.int32).astype(jnp.float32)
    tails = []
    for core in range(2):
        rows = [stage[pl.ds(j * blocks + core, half, stride=2), :] for j in range(4)]
        tails.append(jnp.concatenate(rows, 0).astype(jnp.bfloat16))
    for owner in range(owners):
        send[owner, 0:each, :] = packed[owner]
        send[owner, each:, :] = tails[owner % 2]


def accumulate(cells, first, weights, counts, wide, columns, accs):
    sources, each, _ = cells.shape
    half = each // 8
    for acc in accs:
        pltpu.matmul_pop(acc)
    place = 0
    for s in range(sources):
        wide[s * each : s * each + each // 2, :] = cells[s, : each // 2, :].astype(jnp.float32)
        wide[s * each + each // 2 : (s + 1) * each, :] = weights[s, weights.shape[1] - each // 2 :, :].astype(jnp.float32)
    for s in range(sources):
        for j, top in enumerate((first, first + half, 4 * half, 5 * half, 6 * half)):
            columns[j, pl.ds(place, half), :] = wide[s * each + top : s * each + top + half, :]
        used = wide[s * each + 7 * half : s * each + 7 * half + 1, :][0, 0].astype(jnp.int32)
        place = place + counts(used)
    for j in range(5):
        columns[j, pl.ds(place, GROUP + 4), :] = jnp.zeros((GROUP + 4, LANES), jnp.float32)
    slots = lax.broadcasted_iota(jnp.int32, (2 * KIDS, LANES), 0).astype(jnp.float32).astype(jnp.bfloat16)
    levels = lax.broadcasted_iota(jnp.int32, (LANES, LANES), 0).astype(jnp.float32).astype(jnp.bfloat16)
    zero = jnp.zeros((), jnp.bfloat16)
    one = jnp.ones((), jnp.bfloat16)

    def spread(row, height):
        return jnp.broadcast_to(row, (height, LANES)).astype(jnp.bfloat16)

    def upper(at):
        halves = []
        for k in range(2):
            grad = spread(columns[2, pl.ds(at + k, 1), :], 2 * KIDS)
            hess = spread(columns[3, pl.ds(at + k, 1), :], 2 * KIDS)
            child = columns[4, pl.ds(at + k, 1), :]
            parts = []
            for f in range(2):
                slot = jnp.where(columns[f, pl.ds(at + k, 1), :] >= LANES, child + KIDS, child)
                hit = spread(slot, 2 * KIDS) == slots
                parts += [jnp.where(hit, grad, zero), jnp.where(hit, hess, zero)]
            halves.append(jnp.concatenate(parts, 0))
        return jnp.concatenate(halves, 1)

    def lower(at):
        halves = []
        for k in range(2):
            parts = []
            for f in range(2):
                cell = columns[f, pl.ds(at + k, 1), :]
                low = spread(jnp.where(cell >= LANES, cell - LANES, cell), LANES)
                parts.append(jnp.where(low == levels, one, zero))
            halves.append(jnp.concatenate(parts, 0))
        return jnp.concatenate(halves, 1).astype(LOW)

    def push(chunk, base):
        pltpu.matmul_push_rhs(lower(base + 2 * chunk), staging_register=(chunk // 2) % 2, mxu_index=chunk % 2, transpose=True)

    def step(i, carry):
        base = i * GROUP
        for chunk in range(GROUP // 2):
            pltpu.matmul_acc_lhs(accs[chunk % 2], upper(base + 2 * chunk), load_staged_rhs=(chunk // 2) % 2)
            push(chunk + 2, base)
        return carry

    push(0, 0)
    push(1, 0)
    lax.fori_loop(0, (place + GROUP - 1) // GROUP, step, 0)
    for acc in accs:
        pltpu.matmul_acc_lhs(acc, jnp.zeros((8 * KIDS, B), jnp.bfloat16), load_staged_rhs=0)
    return pltpu.matmul_pop(accs[0]) + pltpu.matmul_pop(accs[1])


def scoped(steps):
    pl.run_scoped(
        lambda *accs: steps(accs),
        pltpu.ACC(0)((8 * KIDS, B), jnp.float32),
        pltpu.ACC(1)((8 * KIDS, B), jnp.float32),
    )


def first_kernel(recv, partial, wide, columns):
    core = lax.rem(lax.axis_index("rows"), 2)

    def steps(accs):
        total = accumulate(recv, 0, recv, lambda used: (used + 1 - core) >> 1, wide, columns, accs)
        for f in range(2):
            partial[f] = total[f * 4 * KIDS : (f + 1) * 4 * KIDS, f * LANES : (f + 1) * LANES]

    scoped(steps)


def last_kernel(recv, other, partial, code, predictions, hist, new_leaf, new_pred, wide, columns):
    core = lax.rem(lax.axis_index("rows"), 2)

    def steps(accs):
        total = accumulate(recv, recv.shape[1] // 4, other, lambda used: (used + core) >> 1, wide, columns, accs)
        for f in range(2):
            mine = partial[f] + total[f * 4 * KIDS : (f + 1) * 4 * KIDS, f * LANES : (f + 1) * LANES]
            for kind in range(2):
                for high in range(2):
                    top = (kind * 2 + high) * KIDS
                    hist[f, kind, :, high * LANES : (high + 1) * LANES] = mine[top : top + KIDS, :]
            if f == 0:
                sums = [jnp.sum(mine[top : top + KIDS, :] + mine[top + KIDS : top + 2 * KIDS, :], 1, keepdims=True) for top in (0, 2 * KIDS)]
        value = -sums[0] / (sums[1] + 1.0)
        leaves = code[...]
        new_leaf[...] = leaves
        gained = jnp.zeros(leaves.shape, jnp.float32)
        for c in range(KIDS):
            gained = jnp.where(leaves == c, jnp.broadcast_to(value[c : c + 1, :], leaves.shape), gained)
        new_pred[...] = predictions[...] + 0.5 * gained

    scoped(steps)


def body(bins, gradients, hessians, predictions, leaf, split_feature, split_bin, row_counts):
    width, length = bins.shape
    blocks = length // LANES
    owners = lax.axis_size("rows")
    feats = lax.axis_size("feat")
    each = width // owners * blocks
    shape = jax.ShapeDtypeStruct
    tall = lambda x: x.reshape(blocks, LANES)
    here = pl.BlockSpec(memory_space=pltpu.HBM)
    height = 2 * each
    wide = pltpu.VMEM((owners * height, LANES), jnp.float32)
    columns = pltpu.VMEM((5, owners * blocks // 2 + GROUP + 8, LANES), jnp.float32)
    part, packed = pl.pallas_call(
        split_kernel,
        out_shape=(shape((blocks, LANES), jnp.bfloat16), shape((owners, each, LANES), jnp.bfloat16)),
        in_specs=[here] * 4,
        out_specs=(VMEM, VMEM),
        scratch_shapes=[
            pltpu.VMEM((width, length), jnp.int32),
            pltpu.VMEM((width * blocks, LANES), jnp.int32),
            pltpu.VMEM((blocks, LANES), jnp.int32),
            pltpu.SMEM((LEAVES,), jnp.int32),
            pltpu.SMEM((LEAVES,), jnp.int32),
            pltpu.SemaphoreType.DMA((3 + width // 8,)),
        ],
        name="split_rows",
        compiler_params=SMALL,
    )(*(pltpu.with_memory_space_constraint(x, pltpu.HBM) for x in (bins, tall(leaf), split_feature, split_bin)))
    others = [lax.ppermute(part, "feat", [(i, (i + s) % feats) for i in range(feats)]) for s in (2, 1, 3)]
    send, code = pl.pallas_call(
        fill_kernel,
        out_shape=(shape((owners, height, LANES), jnp.bfloat16), shape((blocks, LANES), jnp.int32)),
        in_specs=[SMEM] + [VMEM] * 7,
        out_specs=(VMEM, VMEM),
        scratch_shapes=[pltpu.VMEM((4 * blocks, LANES), jnp.float32)],
        name="fill_messages",
        compiler_params=SMALL,
    )(row_counts, packed, tall(gradients), tall(hessians), part, *others)
    recv = lax.all_to_all(send, "rows", 0, 0, tiled=True)
    other = lax.ppermute(recv[:, each:, :], "rows", [(i, i ^ 1) for i in range(owners)])
    partial = pl.pallas_call(
        first_kernel,
        out_shape=shape((2, 4 * KIDS, LANES), jnp.float32),
        in_specs=[VMEM],
        out_specs=VMEM,
        scratch_shapes=[wide, columns],
        name="first_half",
        cost_estimate=pl.CostEstimate(flops=1 << 30, transcendentals=0, bytes_accessed=1 << 20),
        compiler_params=SMALL,
    )(recv)
    hist, new_leaf, new_pred = pl.pallas_call(
        last_kernel,
        out_shape=(shape((2, 2, KIDS, B), jnp.float32), shape((blocks, LANES), jnp.int32), shape((blocks, LANES), jnp.float32)),
        in_specs=[VMEM] * 5,
        out_specs=(VMEM, VMEM, VMEM),
        scratch_shapes=[wide, columns],
        name="histograms",
        compiler_params=SMALL,
    )(recv, other, partial, code, tall(predictions))
    return (hist[None], new_leaf.reshape(-1), new_pred.reshape(-1))


def solution(mesh):
    in_specs = (P("feat", "rows"), P("rows"), P("rows"), P("rows"), P("rows"), P(), P(), P("rows"))
    out_specs = (P("feat", "rows", None, None, None), P("rows"), P("rows"))
    return jax.shard_map(body, mesh=mesh, in_specs=in_specs, out_specs=out_specs, check_vma=False)
```

```python
import jax
import jax.numpy as jnp
from jax import lax
from jax.experimental import pallas as pl
from jax.experimental.pallas import tpu as pltpu
from jax.sharding import PartitionSpec as P

B = 256
LEAVES = 8
KIDS = 2 * LEAVES
LANES = 128
GROUP = 16
LOW = jnp.float8_e4m3fn
VMEM = pl.BlockSpec(memory_space=pltpu.VMEM)
SMALL = pltpu.CompilerParams(vmem_limit_bytes=16 << 20)
SMEM = pl.BlockSpec(memory_space=pltpu.SMEM)


def split_kernel(bins, leaf, features, cutoffs, part, packed, cells, rows, leaves, wanted, limits, sems):
    width, length = bins.shape
    blocks = length // LANES
    copies = [(features, wanted), (cutoffs, limits), (leaf, leaves)]
    copies += [(bins.at[pl.ds(top, 8), :], cells.at[pl.ds(top, 8), :]) for top in range(0, width, 8)]
    copies = [pltpu.make_async_copy(source, target, sems.at[i]) for i, (source, target) in enumerate(copies)]
    for copy in copies:
        copy.start()
    for copy in copies:
        copy.wait()
    for top in range(0, width, 8):
        for k in range(blocks):
            rows[pl.ds(top * blocks + k, 8, stride=blocks), :] = cells[top : top + 8, k * LANES : (k + 1) * LANES]
    first = lax.axis_index("feat") * width
    code = jnp.zeros((blocks, LANES), jnp.int32)
    for slot in range(LEAVES):
        local = wanted[slot] - first
        here = ((local >= 0) & (local < width)).astype(jnp.int32)
        chosen = rows[pl.ds(jnp.clip(local, 0, width - 1) * blocks, blocks), :]
        child = (2 * slot + (chosen > limits[slot]).astype(jnp.int32)) * here
        code = jnp.where(leaves[...] == slot, child, code)
    part[...] = code.astype(jnp.float32).astype(jnp.bfloat16)
    owners, each, _ = packed.shape
    half = blocks // 2
    for owner in range(owners):
        order = [(parity, top) for parity in (owner % 2, 1 - owner % 2) for top in range(owner * each, (owner + 1) * each, blocks)]
        picked = [rows[pl.ds(top + parity, half, stride=2), :].astype(jnp.float32) for parity, top in order]
        packed[owner] = jnp.concatenate(picked, 0).astype(jnp.bfloat16)


def fill_kernel(count, packed, gradients, hessians, mine, one, two, three, send, code, stage):
    owners, each, _ = packed.shape
    blocks = mine.shape[0]
    half = blocks // 2
    total = sum(x[...].astype(jnp.float32) for x in (mine, one, two, three))
    code[...] = total.astype(jnp.int32)
    spot = lax.broadcasted_iota(jnp.int32, (blocks, LANES), 0) * LANES
    spot = spot + lax.broadcasted_iota(jnp.int32, (blocks, LANES), 1)
    live = spot < count[0]
    used = (count[0] + LANES - 1) // LANES
    stage[0:blocks, :] = jnp.where(live, gradients[...].astype(jnp.float32), 0.0)
    stage[blocks : 2 * blocks, :] = jnp.where(live, hessians[...].astype(jnp.float32), 0.0)
    stage[2 * blocks : 3 * blocks, :] = total
    stage[3 * blocks : 4 * blocks, :] = jnp.full((blocks, LANES), used, jnp.int32).astype(jnp.float32)
    tails = []
    for core in range(2):
        rows = [stage[pl.ds(j * blocks + core, half, stride=2), :] for j in range(4)]
        tails.append(jnp.concatenate(rows, 0).astype(jnp.bfloat16))
    for owner in range(owners):
        send[owner, 0:each, :] = packed[owner]
        send[owner, each:, :] = tails[owner % 2]


def accumulate(cells, first, weights, counts, wide, columns, accs):
    sources, each, _ = cells.shape
    half = each // 8
    for acc in accs:
        pltpu.matmul_pop(acc)
    place = 0
    for s in range(sources):
        wide[s * each : s * each + each // 2, :] = cells[s, : each // 2, :].astype(jnp.float32)
        wide[s * each + each // 2 : (s + 1) * each, :] = weights[s, weights.shape[1] - each // 2 :, :].astype(jnp.float32)
    for s in range(sources):
        for j, top in enumerate((first, first + half, 4 * half, 5 * half, 6 * half)):
            columns[j, pl.ds(place, half), :] = wide[s * each + top : s * each + top + half, :]
        used = wide[s * each + 7 * half : s * each + 7 * half + 1, :][0, 0].astype(jnp.int32)
        place = place + counts(used)
    for j in range(5):
        columns[j, pl.ds(place, GROUP + 4), :] = jnp.zeros((GROUP + 4, LANES), jnp.float32)
    slots = lax.broadcasted_iota(jnp.int32, (2 * KIDS, LANES), 0).astype(jnp.float32).astype(jnp.bfloat16)
    levels = lax.broadcasted_iota(jnp.int32, (LANES, LANES), 0).astype(jnp.float32).astype(jnp.bfloat16)
    zero = jnp.zeros((), jnp.bfloat16)
    one = jnp.ones((), jnp.bfloat16)

    def spread(row, height):
        return jnp.broadcast_to(row, (height, LANES)).astype(jnp.bfloat16)

    def upper(at):
        halves = []
        for k in range(2):
            grad = spread(columns[2, pl.ds(at + k, 1), :], 2 * KIDS)
            hess = spread(columns[3, pl.ds(at + k, 1), :], 2 * KIDS)
            child = columns[4, pl.ds(at + k, 1), :]
            parts = []
            for f in range(2):
                slot = jnp.where(columns[f, pl.ds(at + k, 1), :] >= LANES, child + KIDS, child)
                hit = spread(slot, 2 * KIDS) == slots
                parts += [jnp.where(hit, grad, zero), jnp.where(hit, hess, zero)]
            halves.append(jnp.concatenate(parts, 0))
        return jnp.concatenate(halves, 1)

    def lower(at):
        halves = []
        for k in range(2):
            parts = []
            for f in range(2):
                cell = columns[f, pl.ds(at + k, 1), :]
                low = spread(jnp.where(cell >= LANES, cell - LANES, cell), LANES)
                parts.append(jnp.where(low == levels, one, zero))
            halves.append(jnp.concatenate(parts, 0))
        return jnp.concatenate(halves, 1).astype(LOW)

    def push(chunk, base):
        pltpu.matmul_push_rhs(lower(base + 2 * chunk), staging_register=(chunk // 2) % 2, mxu_index=chunk % 2, transpose=True)

    def step(i, carry):
        base = i * GROUP
        for chunk in range(GROUP // 2):
            pltpu.matmul_acc_lhs(accs[chunk % 2], upper(base + 2 * chunk), load_staged_rhs=(chunk // 2) % 2)
            push(chunk + 2, base)
        return carry

    push(0, 0)
    push(1, 0)
    lax.fori_loop(0, (place + GROUP - 1) // GROUP, step, 0)
    for acc in accs:
        pltpu.matmul_acc_lhs(acc, jnp.zeros((8 * KIDS, B), jnp.bfloat16), load_staged_rhs=0)
    return pltpu.matmul_pop(accs[0]) + pltpu.matmul_pop(accs[1])


def scoped(steps):
    pl.run_scoped(
        lambda *accs: steps(accs),
        pltpu.ACC(0)((8 * KIDS, B), jnp.float32),
        pltpu.ACC(1)((8 * KIDS, B), jnp.float32),
    )


def first_kernel(recv, partial, wide, columns):
    core = lax.rem(lax.axis_index("rows"), 2)

    def steps(accs):
        total = accumulate(recv, 0, recv, lambda used: (used + 1 - core) >> 1, wide, columns, accs)
        for f in range(2):
            partial[f] = total[f * 4 * KIDS : (f + 1) * 4 * KIDS, f * LANES : (f + 1) * LANES]

    scoped(steps)


def last_kernel(recv, other, partial, code, predictions, hist, new_leaf, new_pred, wide, columns):
    core = lax.rem(lax.axis_index("rows"), 2)

    def steps(accs):
        total = accumulate(recv, recv.shape[1] // 4, other, lambda used: (used + core) >> 1, wide, columns, accs)
        for f in range(2):
            mine = partial[f] + total[f * 4 * KIDS : (f + 1) * 4 * KIDS, f * LANES : (f + 1) * LANES]
            for kind in range(2):
                for high in range(2):
                    top = (kind * 2 + high) * KIDS
                    hist[f, kind, :, high * LANES : (high + 1) * LANES] = mine[top : top + KIDS, :]
            if f == 0:
                sums = [jnp.sum(mine[top : top + KIDS, :] + mine[top + KIDS : top + 2 * KIDS, :], 1, keepdims=True) for top in (0, 2 * KIDS)]
        value = -sums[0] / (sums[1] + 1.0)
        leaves = code[...]
        new_leaf[...] = leaves
        gained = jnp.zeros(leaves.shape, jnp.float32)
        for c in range(KIDS):
            gained = jnp.where(leaves == c, jnp.broadcast_to(value[c : c + 1, :], leaves.shape), gained)
        new_pred[...] = predictions[...] + 0.5 * gained

    scoped(steps)


def body(bins, gradients, hessians, predictions, leaf, split_feature, split_bin, row_counts):
    width, length = bins.shape
    blocks = length // LANES
    owners = lax.axis_size("rows")
    feats = lax.axis_size("feat")
    each = width // owners * blocks
    shape = jax.ShapeDtypeStruct
    tall = lambda x: x.reshape(blocks, LANES)
    here = pl.BlockSpec(memory_space=pltpu.HBM)
    height = 2 * each
    wide = pltpu.VMEM((owners * height + 8, LANES), jnp.float32)
    columns = pltpu.VMEM((5, owners * blocks // 2 + GROUP + 16, LANES), jnp.float32)
    part, packed = pl.pallas_call(
        split_kernel,
        out_shape=(shape((blocks, LANES), jnp.bfloat16), shape((owners, each, LANES), jnp.bfloat16)),
        in_specs=[here] * 4,
        out_specs=(VMEM, VMEM),
        scratch_shapes=[
            pltpu.VMEM((width, length), jnp.int32),
            pltpu.VMEM((width * blocks + 8, LANES), jnp.int32),
            pltpu.VMEM((blocks, LANES), jnp.int32),
            pltpu.SMEM((LEAVES,), jnp.int32),
            pltpu.SMEM((LEAVES,), jnp.int32),
            pltpu.SemaphoreType.DMA((3 + width // 8,)),
        ],
        name="split_rows",
        compiler_params=SMALL,
    )(*(pltpu.with_memory_space_constraint(x, pltpu.HBM) for x in (bins, tall(leaf), split_feature, split_bin)))
    others = [lax.ppermute(part, "feat", [(i, (i + s) % feats) for i in range(feats)]) for s in (2, 1, 3)]
    send, code = pl.pallas_call(
        fill_kernel,
        out_shape=(shape((owners, height, LANES), jnp.bfloat16), shape((blocks, LANES), jnp.int32)),
        in_specs=[SMEM] + [VMEM] * 7,
        out_specs=(VMEM, VMEM),
        scratch_shapes=[pltpu.VMEM((4 * blocks + 8, LANES), jnp.float32)],
        name="fill_messages",
        compiler_params=SMALL,
    )(row_counts, packed, tall(gradients), tall(hessians), part, *others)
    recv = lax.all_to_all(send, "rows", 0, 0, tiled=True)
    other = lax.ppermute(recv[:, each:, :], "rows", [(i, i ^ 1) for i in range(owners)])
    partial = pl.pallas_call(
        first_kernel,
        out_shape=shape((2, 4 * KIDS, LANES), jnp.float32),
        in_specs=[VMEM],
        out_specs=VMEM,
        scratch_shapes=[wide, columns],
        name="first_half",
        cost_estimate=pl.CostEstimate(flops=1 << 30, transcendentals=0, bytes_accessed=1 << 20),
        compiler_params=SMALL,
    )(recv)
    hist, new_leaf, new_pred = pl.pallas_call(
        last_kernel,
        out_shape=(shape((2, 2, KIDS, B), jnp.float32), shape((blocks, LANES), jnp.int32), shape((blocks, LANES), jnp.float32)),
        in_specs=[VMEM] * 5,
        out_specs=(VMEM, VMEM, VMEM),
        scratch_shapes=[wide, columns],
        name="histograms",
        compiler_params=SMALL,
    )(recv, other, partial, code, tall(predictions))
    return (hist[None], new_leaf.reshape(-1), new_pred.reshape(-1))


def solution(mesh):
    in_specs = (P("feat", "rows"), P("rows"), P("rows"), P("rows"), P("rows"), P(), P(), P("rows"))
    out_specs = (P("feat", "rows", None, None, None), P("rows"), P("rows"))
    return jax.shard_map(body, mesh=mesh, in_specs=in_specs, out_specs=out_specs, check_vma=False)
```

```python
import jax
import jax.numpy as jnp
from jax import lax
from jax.experimental import pallas as pl
from jax.experimental.pallas import tpu as pltpu
from jax.sharding import PartitionSpec as P

B = 256
LEAVES = 8
KIDS = 2 * LEAVES
LANES = 128
GROUP = 16
DEAD = 64.0
LOW = jnp.float8_e4m3fn
VMEM = pl.BlockSpec(memory_space=pltpu.VMEM)
SMALL = pltpu.CompilerParams(vmem_limit_bytes=16 << 20)
SMEM = pl.BlockSpec(memory_space=pltpu.SMEM)


def split_kernel(bins, leaf, features, cutoffs, part, packed, cells, rows, leaves, wanted, limits, sems):
    width, length = bins.shape
    blocks = length // LANES
    copies = [(features, wanted), (cutoffs, limits), (leaf, leaves)]
    copies += [(bins.at[pl.ds(top, 8), :], cells.at[pl.ds(top, 8), :]) for top in range(0, width, 8)]
    copies = [pltpu.make_async_copy(source, target, sems.at[i]) for i, (source, target) in enumerate(copies)]
    for copy in copies:
        copy.start()
    for copy in copies:
        copy.wait()
    for top in range(0, width, 8):
        for k in range(blocks):
            rows[pl.ds(top * blocks + k, 8, stride=blocks), :] = cells[top : top + 8, k * LANES : (k + 1) * LANES]
    first = lax.axis_index("feat") * width
    code = jnp.zeros((blocks, LANES), jnp.int32)
    for slot in range(LEAVES):
        local = wanted[slot] - first
        here = ((local >= 0) & (local < width)).astype(jnp.int32)
        chosen = rows[pl.ds(jnp.clip(local, 0, width - 1) * blocks, blocks), :]
        child = (2 * slot + (chosen > limits[slot]).astype(jnp.int32)) * here
        code = jnp.where(leaves[...] == slot, child, code)
    part[...] = code.astype(jnp.float32).astype(jnp.bfloat16)
    owners, each, _ = packed.shape
    for owner in range(owners):
        core = owner % 2
        order = [(start, top) for start in (2 * core, 1, 2 - 2 * core) for top in range(owner * each, (owner + 1) * each, blocks)]
        picked = [rows[pl.ds(top + start, blocks // 3, stride=3), :].astype(jnp.float32) for start, top in order]
        packed[owner] = jnp.concatenate(picked, 0).astype(jnp.bfloat16)


def fill_kernel(count, packed, gradients, hessians, mine, one, two, three, send, code, stage):
    owners, each, _ = packed.shape
    blocks = mine.shape[0]
    total = sum(x[...].astype(jnp.float32) for x in (mine, one, two, three))
    code[...] = total.astype(jnp.int32)
    spot = lax.broadcasted_iota(jnp.int32, (blocks, LANES), 0) * LANES
    spot = spot + lax.broadcasted_iota(jnp.int32, (blocks, LANES), 1)
    live = spot < count[0]
    stage[0:blocks, :] = gradients[...].astype(jnp.float32)
    stage[blocks : 2 * blocks, :] = hessians[...].astype(jnp.float32)
    stage[2 * blocks : 3 * blocks, :] = jnp.where(live, total, DEAD)
    tails = []
    for core in range(2):
        rows = [stage[pl.ds(j * blocks + start, blocks // 3, stride=3), :] for start in (2 * core, 1) for j in range(3)]
        tails.append(jnp.concatenate(rows, 0).astype(jnp.bfloat16))
    for owner in range(owners):
        send[owner, 0:each, :] = packed[owner]
        send[owner, each:, :] = tails[owner % 2]


def accumulate(lists, size, sources, each, wide, tally, columns, accs):
    for acc in accs:
        pltpu.matmul_pop(acc)
    for n, tops in enumerate(lists):
        alive = jnp.zeros((sources, LANES), jnp.float32)
        for k in range(size):
            kids = wide[pl.ds(tops[4] + k, sources, stride=each), :]
            alive += jnp.where(kids < DEAD, 1.0, 0.0)
        tally[n * sources : (n + 1) * sources, :] = alive
    place = 0
    for s in range(sources):
        for n, tops in enumerate(lists):
            for j, top in enumerate(tops):
                columns[j, pl.ds(place, size), :] = wide[s * each + top : s * each + top + size, :]
            row = n * sources + s
            place = place + tally[row : row + 1, :][0, 0].astype(jnp.int32)
    for j in range(5):
        columns[j, pl.ds(place, GROUP + 4), :] = jnp.zeros((GROUP + 4, LANES), jnp.float32)
    slots = lax.broadcasted_iota(jnp.int32, (2 * KIDS, LANES), 0).astype(jnp.float32).astype(jnp.bfloat16)
    levels = lax.broadcasted_iota(jnp.int32, (LANES, LANES), 0).astype(jnp.float32).astype(jnp.bfloat16)
    zero = jnp.zeros((), jnp.bfloat16)
    one = jnp.ones((), jnp.bfloat16)

    def spread(row, height):
        return jnp.broadcast_to(row, (height, LANES)).astype(jnp.bfloat16)

    def upper(at):
        halves = []
        for k in range(2):
            grad = spread(columns[2, pl.ds(at + k, 1), :], 2 * KIDS)
            hess = spread(columns[3, pl.ds(at + k, 1), :], 2 * KIDS)
            child = columns[4, pl.ds(at + k, 1), :]
            parts = []
            for f in range(2):
                slot = jnp.where(columns[f, pl.ds(at + k, 1), :] >= LANES, child + KIDS, child)
                hit = spread(slot, 2 * KIDS) == slots
                parts += [jnp.where(hit, grad, zero), jnp.where(hit, hess, zero)]
            halves.append(jnp.concatenate(parts, 0))
        return jnp.concatenate(halves, 1)

    def lower(at):
        halves = []
        for k in range(2):
            parts = []
            for f in range(2):
                cell = columns[f, pl.ds(at + k, 1), :]
                low = spread(jnp.where(cell >= LANES, cell - LANES, cell), LANES)
                parts.append(jnp.where(low == levels, one, zero))
            halves.append(jnp.concatenate(parts, 0))
        return jnp.concatenate(halves, 1).astype(LOW)

    def push(chunk, base):
        pltpu.matmul_push_rhs(lower(base + 2 * chunk), staging_register=(chunk // 2) % 2, mxu_index=chunk % 2, transpose=True)

    def step(i, carry):
        base = i * GROUP
        for chunk in range(GROUP // 2):
            pltpu.matmul_acc_lhs(accs[chunk % 2], upper(base + 2 * chunk), load_staged_rhs=(chunk // 2) % 2)
            push(chunk + 2, base)
        return carry

    push(0, 0)
    push(1, 0)
    lax.fori_loop(0, (place + GROUP - 1) // GROUP, step, 0)
    for acc in accs:
        pltpu.matmul_acc_lhs(acc, jnp.zeros((8 * KIDS, B), jnp.bfloat16), load_staged_rhs=0)
    return pltpu.matmul_pop(accs[0]) + pltpu.matmul_pop(accs[1])


def scoped(steps):
    pl.run_scoped(
        lambda *accs: steps(accs),
        pltpu.ACC(0)((8 * KIDS, B), jnp.float32),
        pltpu.ACC(1)((8 * KIDS, B), jnp.float32),
    )


def first_kernel(recv, partial, wide, tally, columns):
    sources, each, _ = recv.shape
    size = each // 12

    def steps(accs):
        for s in range(sources):
            wide[s * each : (s + 1) * each, :] = recv[s].astype(jnp.float32)
        lists = [tuple(size * k for k in (0, 1, 6, 7, 8)), tuple(size * k for k in (2, 3, 9, 10, 11))]
        total = accumulate(lists, size, sources, each, wide, tally, columns, accs)
        for f in range(2):
            partial[f] = total[f * 4 * KIDS : (f + 1) * 4 * KIDS, f * LANES : (f + 1) * LANES]

    scoped(steps)


def last_kernel(recv, other, partial, code, predictions, hist, new_leaf, new_pred, wide, tally, columns):
    sources, each, _ = recv.shape
    size = each // 12

    def steps(accs):
        for s in range(sources):
            top = s * 6 * size
            wide[top : top + 2 * size, :] = recv[s, 4 * size : 6 * size, :].astype(jnp.float32)
            wide[top + 2 * size : top + 5 * size, :] = other[s].astype(jnp.float32)
        lists = [tuple(size * k for k in (0, 1, 2, 3, 4))]
        total = accumulate(lists, size, sources, 6 * size, wide, tally, columns, accs)
        for f in range(2):
            mine = partial[f] + total[f * 4 * KIDS : (f + 1) * 4 * KIDS, f * LANES : (f + 1) * LANES]
            for kind in range(2):
                for high in range(2):
                    top = (kind * 2 + high) * KIDS
                    hist[f, kind, :, high * LANES : (high + 1) * LANES] = mine[top : top + KIDS, :]
            if f == 0:
                sums = [jnp.sum(mine[top : top + KIDS, :] + mine[top + KIDS : top + 2 * KIDS, :], 1, keepdims=True) for top in (0, 2 * KIDS)]
        value = -sums[0] / (sums[1] + 1.0)
        leaves = code[...]
        new_leaf[...] = leaves
        gained = jnp.zeros(leaves.shape, jnp.float32)
        for c in range(KIDS):
            gained = jnp.where(leaves == c, jnp.broadcast_to(value[c : c + 1, :], leaves.shape), gained)
        new_pred[...] = predictions[...] + 0.5 * gained

    scoped(steps)


def body(bins, gradients, hessians, predictions, leaf, split_feature, split_bin, row_counts):
    width, length = bins.shape
    blocks = length // LANES
    owners = lax.axis_size("rows")
    feats = lax.axis_size("feat")
    each = width // owners * blocks
    shape = jax.ShapeDtypeStruct
    tall = lambda x: x.reshape(blocks, LANES)
    here = pl.BlockSpec(memory_space=pltpu.HBM)
    height = 2 * each
    tally = pltpu.VMEM((2 * owners, LANES), jnp.float32)
    columns = pltpu.VMEM((5, owners * blocks * 2 // 3 + GROUP + 16, LANES), jnp.float32)
    part, packed = pl.pallas_call(
        split_kernel,
        out_shape=(shape((blocks, LANES), jnp.bfloat16), shape((owners, each, LANES), jnp.bfloat16)),
        in_specs=[here] * 4,
        out_specs=(VMEM, VMEM),
        scratch_shapes=[
            pltpu.VMEM((width, length), jnp.int32),
            pltpu.VMEM((width * blocks + 8, LANES), jnp.int32),
            pltpu.VMEM((blocks, LANES), jnp.int32),
            pltpu.SMEM((LEAVES,), jnp.int32),
            pltpu.SMEM((LEAVES,), jnp.int32),
            pltpu.SemaphoreType.DMA((3 + width // 8,)),
        ],
        name="split_rows",
        compiler_params=SMALL,
    )(*(pltpu.with_memory_space_constraint(x, pltpu.HBM) for x in (bins, tall(leaf), split_feature, split_bin)))
    others = [lax.ppermute(part, "feat", [(i, (i + s) % feats) for i in range(feats)]) for s in (3, 1, 2)]
    send, code = pl.pallas_call(
        fill_kernel,
        out_shape=(shape((owners, height, LANES), jnp.bfloat16), shape((blocks, LANES), jnp.int32)),
        in_specs=[SMEM] + [VMEM] * 7,
        out_specs=(VMEM, VMEM),
        scratch_shapes=[pltpu.VMEM((4 * blocks + 8, LANES), jnp.float32)],
        name="fill_messages",
        compiler_params=SMALL,
    )(row_counts, packed, tall(gradients), tall(hessians), part, *others)
    recv = lax.all_to_all(send, "rows", 0, 0, tiled=True)
    other = lax.ppermute(recv[:, each : each + blocks, :], "rows", [(i, i ^ 1) for i in range(owners)])
    partial = pl.pallas_call(
        first_kernel,
        out_shape=shape((2, 4 * KIDS, LANES), jnp.float32),
        in_specs=[VMEM],
        out_specs=VMEM,
        scratch_shapes=[pltpu.VMEM((owners * height + 8, LANES), jnp.float32), tally, columns],
        name="first_half",
        cost_estimate=pl.CostEstimate(flops=1 << 30, transcendentals=0, bytes_accessed=1 << 20),
        compiler_params=SMALL,
    )(recv)
    hist, new_leaf, new_pred = pl.pallas_call(
        last_kernel,
        out_shape=(shape((2, 2, KIDS, B), jnp.float32), shape((blocks, LANES), jnp.int32), shape((blocks, LANES), jnp.float32)),
        in_specs=[VMEM] * 5,
        out_specs=(VMEM, VMEM, VMEM),
        scratch_shapes=[pltpu.VMEM((owners * each + 8, LANES), jnp.float32), tally, columns],
        name="histograms",
        compiler_params=SMALL,
    )(recv, other, partial, code, tall(predictions))
    return (hist[None], new_leaf.reshape(-1), new_pred.reshape(-1))


def solution(mesh):
    in_specs = (P("feat", "rows"), P("rows"), P("rows"), P("rows"), P("rows"), P(), P(), P("rows"))
    out_specs = (P("feat", "rows", None, None, None), P("rows"), P("rows"))
    return jax.shard_map(body, mesh=mesh, in_specs=in_specs, out_specs=out_specs, check_vma=False)
```

```python
import jax
import jax.numpy as jnp
from jax import lax
from jax.experimental import pallas as pl
from jax.experimental.pallas import tpu as pltpu
from jax.sharding import PartitionSpec as P

B = 256
LEAVES = 8
KIDS = 2 * LEAVES
LANES = 128
GROUP = 16
DEAD = 64.0
LOW = jnp.float8_e4m3fn
VMEM = pl.BlockSpec(memory_space=pltpu.VMEM)
SMALL = pltpu.CompilerParams(vmem_limit_bytes=16 << 20)
SMEM = pl.BlockSpec(memory_space=pltpu.SMEM)


def split_kernel(bins, leaf, features, cutoffs, part, rows, cells, leaves, wanted, limits, sems):
    width, length = bins.shape
    blocks = length // LANES
    copies = [(features, wanted), (cutoffs, limits), (leaf, leaves)]
    copies += [(bins.at[pl.ds(top, 8), :], cells.at[pl.ds(top, 8), :]) for top in range(0, width, 8)]
    copies = [pltpu.make_async_copy(source, target, sems.at[i]) for i, (source, target) in enumerate(copies)]
    for copy in copies:
        copy.start()
    for copy in copies:
        copy.wait()
    for top in range(0, width, 8):
        for k in range(blocks):
            rows[pl.ds(top * blocks + k, 8, stride=blocks), :] = cells[top : top + 8, k * LANES : (k + 1) * LANES]
    first = lax.axis_index("feat") * width
    code = jnp.zeros((blocks, LANES), jnp.int32)
    for slot in range(LEAVES):
        local = wanted[slot] - first
        here = ((local >= 0) & (local < width)).astype(jnp.int32)
        chosen = rows[pl.ds(jnp.clip(local, 0, width - 1) * blocks, blocks), :]
        child = (2 * slot + (chosen > limits[slot]).astype(jnp.int32)) * here
        code = jnp.where(leaves[...] == slot, child, code)
    part[...] = code.astype(jnp.float32).astype(jnp.bfloat16)


def pack_kernel(rows, packed):
    blocks = packed.shape[1] // 2
    owners, each, _ = packed.shape
    for owner in range(owners):
        core = owner % 2
        order = [(start, top) for start in (2 * core, 1, 2 - 2 * core) for top in range(owner * each, (owner + 1) * each, blocks)]
        picked = [rows[pl.ds(top + start, blocks // 3, stride=3), :].astype(jnp.float32) for start, top in order]
        packed[owner] = jnp.concatenate(picked, 0).astype(jnp.bfloat16)


def fill_kernel(count, packed, gradients, hessians, mine, one, two, three, send, code, stage):
    owners, each, _ = packed.shape
    blocks = mine.shape[0]
    total = sum(x[...].astype(jnp.float32) for x in (mine, one, two, three))
    code[...] = total.astype(jnp.int32)
    spot = lax.broadcasted_iota(jnp.int32, (blocks, LANES), 0) * LANES
    spot = spot + lax.broadcasted_iota(jnp.int32, (blocks, LANES), 1)
    live = spot < count[0]
    stage[0:blocks, :] = gradients[...].astype(jnp.float32)
    stage[blocks : 2 * blocks, :] = hessians[...].astype(jnp.float32)
    stage[2 * blocks : 3 * blocks, :] = jnp.where(live, total, DEAD)
    tails = []
    for core in range(2):
        rows = [stage[pl.ds(j * blocks + start, blocks // 3, stride=3), :] for start in (2 * core, 1) for j in range(3)]
        tails.append(jnp.concatenate(rows, 0).astype(jnp.bfloat16))
    for owner in range(owners):
        send[owner, 0:each, :] = packed[owner]
        send[owner, each:, :] = tails[owner % 2]


def accumulate(lists, size, sources, each, wide, tally, columns, accs):
    for acc in accs:
        pltpu.matmul_pop(acc)
    for n, tops in enumerate(lists):
        alive = jnp.zeros((sources, LANES), jnp.float32)
        for k in range(size):
            kids = wide[pl.ds(tops[4] + k, sources, stride=each), :]
            alive += jnp.where(kids < DEAD, 1.0, 0.0)
        tally[n * sources : (n + 1) * sources, :] = alive
    place = 0
    for s in range(sources):
        for n, tops in enumerate(lists):
            for j, top in enumerate(tops):
                columns[j, pl.ds(place, size), :] = wide[s * each + top : s * each + top + size, :]
            row = n * sources + s
            place = place + tally[row : row + 1, :][0, 0].astype(jnp.int32)
    for j in range(5):
        columns[j, pl.ds(place, GROUP + 4), :] = jnp.zeros((GROUP + 4, LANES), jnp.float32)
    slots = lax.broadcasted_iota(jnp.int32, (2 * KIDS, LANES), 0).astype(jnp.float32).astype(jnp.bfloat16)
    levels = lax.broadcasted_iota(jnp.int32, (LANES, LANES), 0).astype(jnp.float32).astype(jnp.bfloat16)
    zero = jnp.zeros((), jnp.bfloat16)
    one = jnp.ones((), jnp.bfloat16)

    def spread(row, height):
        return jnp.broadcast_to(row, (height, LANES)).astype(jnp.bfloat16)

    def upper(at):
        halves = []
        for k in range(2):
            grad = spread(columns[2, pl.ds(at + k, 1), :], 2 * KIDS)
            hess = spread(columns[3, pl.ds(at + k, 1), :], 2 * KIDS)
            child = columns[4, pl.ds(at + k, 1), :]
            parts = []
            for f in range(2):
                slot = jnp.where(columns[f, pl.ds(at + k, 1), :] >= LANES, child + KIDS, child)
                hit = spread(slot, 2 * KIDS) == slots
                parts += [jnp.where(hit, grad, zero), jnp.where(hit, hess, zero)]
            halves.append(jnp.concatenate(parts, 0))
        return jnp.concatenate(halves, 1)

    def lower(at):
        halves = []
        for k in range(2):
            parts = []
            for f in range(2):
                cell = columns[f, pl.ds(at + k, 1), :]
                low = spread(jnp.where(cell >= LANES, cell - LANES, cell), LANES)
                parts.append(jnp.where(low == levels, one, zero))
            halves.append(jnp.concatenate(parts, 0))
        return jnp.concatenate(halves, 1).astype(LOW)

    def push(chunk, base):
        pltpu.matmul_push_rhs(lower(base + 2 * chunk), staging_register=(chunk // 2) % 2, mxu_index=chunk % 2, transpose=True)

    def step(i, carry):
        base = i * GROUP
        for chunk in range(GROUP // 2):
            pltpu.matmul_acc_lhs(accs[chunk % 2], upper(base + 2 * chunk), load_staged_rhs=(chunk // 2) % 2)
            push(chunk + 2, base)
        return carry

    push(0, 0)
    push(1, 0)
    lax.fori_loop(0, (place + GROUP - 1) // GROUP, step, 0)
    for acc in accs:
        pltpu.matmul_acc_lhs(acc, jnp.zeros((8 * KIDS, B), jnp.bfloat16), load_staged_rhs=0)
    return pltpu.matmul_pop(accs[0]) + pltpu.matmul_pop(accs[1])


def scoped(steps):
    pl.run_scoped(
        lambda *accs: steps(accs),
        pltpu.ACC(0)((8 * KIDS, B), jnp.float32),
        pltpu.ACC(1)((8 * KIDS, B), jnp.float32),
    )


def first_kernel(recv, partial, wide, tally, columns):
    sources, each, _ = recv.shape
    size = each // 12

    def steps(accs):
        for s in range(sources):
            wide[s * each : (s + 1) * each, :] = recv[s].astype(jnp.float32)
        lists = [tuple(size * k for k in (0, 1, 6, 7, 8)), tuple(size * k for k in (2, 3, 9, 10, 11))]
        total = accumulate(lists, size, sources, each, wide, tally, columns, accs)
        for f in range(2):
            partial[f] = total[f * 4 * KIDS : (f + 1) * 4 * KIDS, f * LANES : (f + 1) * LANES]

    scoped(steps)


def last_kernel(recv, other, partial, code, predictions, hist, new_leaf, new_pred, wide, tally, columns):
    sources, each, _ = recv.shape
    size = each // 12

    def steps(accs):
        for s in range(sources):
            top = s * 6 * size
            wide[top : top + 2 * size, :] = recv[s, 4 * size : 6 * size, :].astype(jnp.float32)
            wide[top + 2 * size : top + 5 * size, :] = other[s].astype(jnp.float32)
        lists = [tuple(size * k for k in (0, 1, 2, 3, 4))]
        total = accumulate(lists, size, sources, 6 * size, wide, tally, columns, accs)
        for f in range(2):
            mine = partial[f] + total[f * 4 * KIDS : (f + 1) * 4 * KIDS, f * LANES : (f + 1) * LANES]
            for kind in range(2):
                for high in range(2):
                    top = (kind * 2 + high) * KIDS
                    hist[f, kind, :, high * LANES : (high + 1) * LANES] = mine[top : top + KIDS, :]
            if f == 0:
                sums = [jnp.sum(mine[top : top + KIDS, :] + mine[top + KIDS : top + 2 * KIDS, :], 1, keepdims=True) for top in (0, 2 * KIDS)]
        value = -sums[0] / (sums[1] + 1.0)
        leaves = code[...]
        new_leaf[...] = leaves
        gained = jnp.zeros(leaves.shape, jnp.float32)
        for c in range(KIDS):
            gained = jnp.where(leaves == c, jnp.broadcast_to(value[c : c + 1, :], leaves.shape), gained)
        new_pred[...] = predictions[...] + 0.5 * gained

    scoped(steps)


def body(bins, gradients, hessians, predictions, leaf, split_feature, split_bin, row_counts):
    width, length = bins.shape
    blocks = length // LANES
    owners = lax.axis_size("rows")
    feats = lax.axis_size("feat")
    each = width // owners * blocks
    shape = jax.ShapeDtypeStruct
    tall = lambda x: x.reshape(blocks, LANES)
    here = pl.BlockSpec(memory_space=pltpu.HBM)
    height = 2 * each
    tally = pltpu.VMEM((2 * owners, LANES), jnp.float32)
    columns = pltpu.VMEM((5, owners * blocks * 2 // 3 + GROUP + 16, LANES), jnp.float32)
    part, spread_out = pl.pallas_call(
        split_kernel,
        out_shape=(shape((blocks, LANES), jnp.bfloat16), shape((width * blocks + 8, LANES), jnp.int32)),
        in_specs=[here] * 4,
        out_specs=(VMEM, VMEM),
        scratch_shapes=[
            pltpu.VMEM((width, length), jnp.int32),
            pltpu.VMEM((blocks, LANES), jnp.int32),
            pltpu.SMEM((LEAVES,), jnp.int32),
            pltpu.SMEM((LEAVES,), jnp.int32),
            pltpu.SemaphoreType.DMA((3 + width // 8,)),
        ],
        name="split_rows",
        compiler_params=SMALL,
    )(*(pltpu.with_memory_space_constraint(x, pltpu.HBM) for x in (bins, tall(leaf), split_feature, split_bin)))
    packed = pl.pallas_call(
        pack_kernel,
        out_shape=shape((owners, each, LANES), jnp.bfloat16),
        in_specs=[VMEM],
        out_specs=VMEM,
        name="pack_bins",
        compiler_params=SMALL,
    )(spread_out)
    others = [lax.ppermute(part, "feat", [(i, (i + s) % feats) for i in range(feats)]) for s in (3, 1, 2)]
    send, code = pl.pallas_call(
        fill_kernel,
        out_shape=(shape((owners, height, LANES), jnp.bfloat16), shape((blocks, LANES), jnp.int32)),
        in_specs=[SMEM] + [VMEM] * 7,
        out_specs=(VMEM, VMEM),
        scratch_shapes=[pltpu.VMEM((4 * blocks + 8, LANES), jnp.float32)],
        name="fill_messages",
        compiler_params=SMALL,
    )(row_counts, packed, tall(gradients), tall(hessians), part, *others)
    recv = lax.all_to_all(send, "rows", 0, 0, tiled=True)
    other = lax.ppermute(recv[:, each : each + blocks, :], "rows", [(i, i ^ 1) for i in range(owners)])
    partial = pl.pallas_call(
        first_kernel,
        out_shape=shape((2, 4 * KIDS, LANES), jnp.float32),
        in_specs=[VMEM],
        out_specs=VMEM,
        scratch_shapes=[pltpu.VMEM((owners * height + 8, LANES), jnp.float32), tally, columns],
        name="first_half",
        cost_estimate=pl.CostEstimate(flops=1 << 30, transcendentals=0, bytes_accessed=1 << 20),
        compiler_params=SMALL,
    )(recv)
    hist, new_leaf, new_pred = pl.pallas_call(
        last_kernel,
        out_shape=(shape((2, 2, KIDS, B), jnp.float32), shape((blocks, LANES), jnp.int32), shape((blocks, LANES), jnp.float32)),
        in_specs=[VMEM] * 5,
        out_specs=(VMEM, VMEM, VMEM),
        scratch_shapes=[pltpu.VMEM((owners * each + 8, LANES), jnp.float32), tally, columns],
        name="histograms",
        compiler_params=SMALL,
    )(recv, other, partial, code, tall(predictions))
    return (hist[None], new_leaf.reshape(-1), new_pred.reshape(-1))


def solution(mesh):
    in_specs = (P("feat", "rows"), P("rows"), P("rows"), P("rows"), P("rows"), P(), P(), P("rows"))
    out_specs = (P("feat", "rows", None, None, None), P("rows"), P("rows"))
    return jax.shard_map(body, mesh=mesh, in_specs=in_specs, out_specs=out_specs, check_vma=False)
```

```python
import jax
import jax.numpy as jnp
from jax import lax
from jax.experimental import pallas as pl
from jax.experimental.pallas import tpu as pltpu
from jax.sharding import PartitionSpec as P

B = 256
LEAVES = 8
KIDS = 2 * LEAVES
LANES = 128
GROUP = 16
LOW = jnp.float8_e4m3fn
VMEM = pl.BlockSpec(memory_space=pltpu.VMEM)
SMALL = pltpu.CompilerParams(vmem_limit_bytes=16 << 20)
SMEM = pl.BlockSpec(memory_space=pltpu.SMEM)


def split_kernel(bins, leaf, features, cutoffs, part, rows, cells, leaves, wanted, limits, sems):
    width, length = bins.shape
    blocks = length // LANES
    copies = [(features, wanted), (cutoffs, limits), (leaf, leaves)]
    copies += [(bins.at[pl.ds(top, 8), :], cells.at[pl.ds(top, 8), :]) for top in range(0, width, 8)]
    copies = [pltpu.make_async_copy(source, target, sems.at[i]) for i, (source, target) in enumerate(copies)]
    for copy in copies:
        copy.start()
    for copy in copies:
        copy.wait()
    for top in range(0, width, 8):
        for k in range(blocks):
            rows[pl.ds(top * blocks + k, 8, stride=blocks), :] = cells[top : top + 8, k * LANES : (k + 1) * LANES]
    first = lax.axis_index("feat") * width
    code = jnp.zeros((blocks, LANES), jnp.int32)
    for slot in range(LEAVES):
        local = wanted[slot] - first
        here = ((local >= 0) & (local < width)).astype(jnp.int32)
        chosen = rows[pl.ds(jnp.clip(local, 0, width - 1) * blocks, blocks), :]
        child = (2 * slot + (chosen > limits[slot]).astype(jnp.int32)) * here
        code = jnp.where(leaves[...] == slot, child, code)
    part[...] = code.astype(jnp.float32).astype(jnp.bfloat16)


def pack_kernel(rows, packed):
    blocks = packed.shape[1] // 2
    owners, each, _ = packed.shape
    half = blocks // 2
    for owner in range(owners):
        order = [(parity, top) for parity in (owner % 2, 1 - owner % 2) for top in range(owner * each, (owner + 1) * each, blocks)]
        picked = [rows[pl.ds(top + parity, half, stride=2), :].astype(jnp.float32) for parity, top in order]
        packed[owner] = jnp.concatenate(picked, 0).astype(jnp.bfloat16)


def fill_kernel(count, packed, gradients, hessians, mine, one, two, three, send, code, stage):
    owners, each, _ = packed.shape
    blocks = mine.shape[0]
    half = blocks // 2
    total = sum(x[...].astype(jnp.float32) for x in (mine, one, two, three))
    code[...] = total.astype(jnp.int32)
    spot = lax.broadcasted_iota(jnp.int32, (blocks, LANES), 0) * LANES
    spot = spot + lax.broadcasted_iota(jnp.int32, (blocks, LANES), 1)
    live = spot < count[0]
    used = (count[0] + LANES - 1) // LANES
    stage[0:blocks, :] = jnp.where(live, gradients[...].astype(jnp.float32), 0.0)
    stage[blocks : 2 * blocks, :] = jnp.where(live, hessians[...].astype(jnp.float32), 0.0)
    stage[2 * blocks : 3 * blocks, :] = total
    stage[3 * blocks : 4 * blocks, :] = jnp.full((blocks, LANES), used, jnp.int32).astype(jnp.float32)
    tails = []
    for core in range(2):
        rows = [stage[pl.ds(j * blocks + core, half, stride=2), :] for j in range(4)]
        tails.append(jnp.concatenate(rows, 0).astype(jnp.bfloat16))
    for owner in range(owners):
        send[owner, 0:each, :] = packed[owner]
        send[owner, each:, :] = tails[owner % 2]


def accumulate(cells, first, weights, counts, wide, columns, accs):
    sources, each, _ = cells.shape
    half = each // 8
    for acc in accs:
        pltpu.matmul_pop(acc)
    place = 0
    for s in range(sources):
        wide[s * each : s * each + each // 2, :] = cells[s, : each // 2, :].astype(jnp.float32)
        wide[s * each + each // 2 : (s + 1) * each, :] = weights[s, weights.shape[1] - each // 2 :, :].astype(jnp.float32)
    for s in range(sources):
        for j, top in enumerate((first, first + half, 4 * half, 5 * half, 6 * half)):
            columns[j, pl.ds(place, half), :] = wide[s * each + top : s * each + top + half, :]
        used = wide[s * each + 7 * half : s * each + 7 * half + 1, :][0, 0].astype(jnp.int32)
        place = place + counts(used)
    for j in range(5):
        columns[j, pl.ds(place, GROUP + 4), :] = jnp.zeros((GROUP + 4, LANES), jnp.float32)
    slots = lax.broadcasted_iota(jnp.int32, (2 * KIDS, LANES), 0).astype(jnp.float32).astype(jnp.bfloat16)
    levels = lax.broadcasted_iota(jnp.int32, (LANES, LANES), 0).astype(jnp.float32).astype(jnp.bfloat16)
    zero = jnp.zeros((), jnp.bfloat16)
    one = jnp.ones((), jnp.bfloat16)

    def spread(row, height):
        return jnp.broadcast_to(row, (height, LANES)).astype(jnp.bfloat16)

    def upper(at):
        halves = []
        for k in range(2):
            grad = spread(columns[2, pl.ds(at + k, 1), :], 2 * KIDS)
            hess = spread(columns[3, pl.ds(at + k, 1), :], 2 * KIDS)
            child = columns[4, pl.ds(at + k, 1), :]
            parts = []
            for f in range(2):
                slot = jnp.where(columns[f, pl.ds(at + k, 1), :] >= LANES, child + KIDS, child)
                hit = spread(slot, 2 * KIDS) == slots
                parts += [jnp.where(hit, grad, zero), jnp.where(hit, hess, zero)]
            halves.append(jnp.concatenate(parts, 0))
        return jnp.concatenate(halves, 1)

    def lower(at):
        halves = []
        for k in range(2):
            parts = []
            for f in range(2):
                cell = columns[f, pl.ds(at + k, 1), :]
                low = spread(jnp.where(cell >= LANES, cell - LANES, cell), LANES)
                parts.append(jnp.where(low == levels, one, zero))
            halves.append(jnp.concatenate(parts, 0))
        return jnp.concatenate(halves, 1).astype(LOW)

    def push(chunk, base):
        pltpu.matmul_push_rhs(lower(base + 2 * chunk), staging_register=(chunk // 2) % 2, mxu_index=chunk % 2, transpose=True)

    def step(i, carry):
        base = i * GROUP
        for chunk in range(GROUP // 2):
            pltpu.matmul_acc_lhs(accs[chunk % 2], upper(base + 2 * chunk), load_staged_rhs=(chunk // 2) % 2)
            push(chunk + 2, base)
        return carry

    push(0, 0)
    push(1, 0)
    lax.fori_loop(0, (place + GROUP - 1) // GROUP, step, 0)
    for acc in accs:
        pltpu.matmul_acc_lhs(acc, jnp.zeros((8 * KIDS, B), jnp.bfloat16), load_staged_rhs=0)
    return pltpu.matmul_pop(accs[0]) + pltpu.matmul_pop(accs[1])


def scoped(steps):
    pl.run_scoped(
        lambda *accs: steps(accs),
        pltpu.ACC(0)((8 * KIDS, B), jnp.float32),
        pltpu.ACC(1)((8 * KIDS, B), jnp.float32),
    )


def first_kernel(recv, partial, wide, columns):
    core = lax.rem(lax.axis_index("rows"), 2)

    def steps(accs):
        total = accumulate(recv, 0, recv, lambda used: (used + 1 - core) >> 1, wide, columns, accs)
        for f in range(2):
            partial[f] = total[f * 4 * KIDS : (f + 1) * 4 * KIDS, f * LANES : (f + 1) * LANES]

    scoped(steps)


def last_kernel(recv, other, partial, code, predictions, hist, new_leaf, new_pred, wide, columns):
    core = lax.rem(lax.axis_index("rows"), 2)

    def steps(accs):
        total = accumulate(recv, recv.shape[1] // 4, other, lambda used: (used + core) >> 1, wide, columns, accs)
        for f in range(2):
            mine = partial[f] + total[f * 4 * KIDS : (f + 1) * 4 * KIDS, f * LANES : (f + 1) * LANES]
            for kind in range(2):
                for high in range(2):
                    top = (kind * 2 + high) * KIDS
                    hist[f, kind, :, high * LANES : (high + 1) * LANES] = mine[top : top + KIDS, :]
            if f == 0:
                sums = [jnp.sum(mine[top : top + KIDS, :] + mine[top + KIDS : top + 2 * KIDS, :], 1, keepdims=True) for top in (0, 2 * KIDS)]
        value = -sums[0] / (sums[1] + 1.0)
        leaves = code[...]
        new_leaf[...] = leaves
        gained = jnp.zeros(leaves.shape, jnp.float32)
        for c in range(KIDS):
            gained = jnp.where(leaves == c, jnp.broadcast_to(value[c : c + 1, :], leaves.shape), gained)
        new_pred[...] = predictions[...] + 0.5 * gained

    scoped(steps)


def body(bins, gradients, hessians, predictions, leaf, split_feature, split_bin, row_counts):
    width, length = bins.shape
    blocks = length // LANES
    owners = lax.axis_size("rows")
    feats = lax.axis_size("feat")
    each = width // owners * blocks
    shape = jax.ShapeDtypeStruct
    tall = lambda x: x.reshape(blocks, LANES)
    here = pl.BlockSpec(memory_space=pltpu.HBM)
    height = 2 * each
    wide = pltpu.VMEM((owners * height + 8, LANES), jnp.float32)
    columns = pltpu.VMEM((5, owners * blocks // 2 + GROUP + 16, LANES), jnp.float32)
    part, spread_out = pl.pallas_call(
        split_kernel,
        out_shape=(shape((blocks, LANES), jnp.bfloat16), shape((width * blocks + 8, LANES), jnp.int32)),
        in_specs=[here] * 4,
        out_specs=(VMEM, VMEM),
        scratch_shapes=[
            pltpu.VMEM((width, length), jnp.int32),
            pltpu.VMEM((blocks, LANES), jnp.int32),
            pltpu.SMEM((LEAVES,), jnp.int32),
            pltpu.SMEM((LEAVES,), jnp.int32),
            pltpu.SemaphoreType.DMA((3 + width // 8,)),
        ],
        name="split_rows",
        compiler_params=SMALL,
    )(*(pltpu.with_memory_space_constraint(x, pltpu.HBM) for x in (bins, tall(leaf), split_feature, split_bin)))
    packed = pl.pallas_call(
        pack_kernel,
        out_shape=shape((owners, each, LANES), jnp.bfloat16),
        in_specs=[VMEM],
        out_specs=VMEM,
        name="pack_bins",
        compiler_params=SMALL,
    )(spread_out)
    others = [lax.ppermute(part, "feat", [(i, (i + s) % feats) for i in range(feats)]) for s in (2, 1, 3)]
    send, code = pl.pallas_call(
        fill_kernel,
        out_shape=(shape((owners, height, LANES), jnp.bfloat16), shape((blocks, LANES), jnp.int32)),
        in_specs=[SMEM] + [VMEM] * 7,
        out_specs=(VMEM, VMEM),
        scratch_shapes=[pltpu.VMEM((4 * blocks + 8, LANES), jnp.float32)],
        name="fill_messages",
        compiler_params=SMALL,
    )(row_counts, packed, tall(gradients), tall(hessians), part, *others)
    recv = lax.all_to_all(send, "rows", 0, 0, tiled=True)
    other = lax.ppermute(recv[:, each:, :], "rows", [(i, i ^ 1) for i in range(owners)])
    partial = pl.pallas_call(
        first_kernel,
        out_shape=shape((2, 4 * KIDS, LANES), jnp.float32),
        in_specs=[VMEM],
        out_specs=VMEM,
        scratch_shapes=[wide, columns],
        name="first_half",
        cost_estimate=pl.CostEstimate(flops=1 << 30, transcendentals=0, bytes_accessed=1 << 20),
        compiler_params=SMALL,
    )(recv)
    hist, new_leaf, new_pred = pl.pallas_call(
        last_kernel,
        out_shape=(shape((2, 2, KIDS, B), jnp.float32), shape((blocks, LANES), jnp.int32), shape((blocks, LANES), jnp.float32)),
        in_specs=[VMEM] * 5,
        out_specs=(VMEM, VMEM, VMEM),
        scratch_shapes=[wide, columns],
        name="histograms",
        compiler_params=SMALL,
    )(recv, other, partial, code, tall(predictions))
    return (hist[None], new_leaf.reshape(-1), new_pred.reshape(-1))


def solution(mesh):
    in_specs = (P("feat", "rows"), P("rows"), P("rows"), P("rows"), P("rows"), P(), P(), P("rows"))
    out_specs = (P("feat", "rows", None, None, None), P("rows"), P("rows"))
    return jax.shard_map(body, mesh=mesh, in_specs=in_specs, out_specs=out_specs, check_vma=False)
```
